8 devices in a mesh: dp: 1 (over z), sp: 8 (over y, x, core).
Axes of the slice: x: 2, y: 2, z: 1, core: 2. Of those that a mesh axis runs over, the one named last changes fastest.
Arguments:
- image_tokens: bfloat16 [32, 1024, 1152], P('dp', 'sp')
- ln1_gain: float32 [2, 1152], replicated
- ln1_shift: float32 [2, 1152], replicated
- w_qkv: bfloat16 [2, 1152, 3, 16, 72], replicated
- b_qkv: float32 [2, 3, 16, 72], replicated
- w_out: bfloat16 [2, 16, 72, 1152], replicated
- b_out: float32 [2, 1152], replicated
- ln2_gain: float32 [2, 1152], replicated
- ln2_shift: float32 [2, 1152], replicated
- w_up: bfloat16 [2, 1152, 4304], replicated
- b_up: float32 [2, 4304], replicated
- w_down: bfloat16 [2, 4304, 1152], replicated
- b_down: float32 [2, 1152], replicated
Outputs:
- output: bfloat16 [32, 1024, 1152], P('dp', 'sp')
All inputs are finite; a program needn't handle non-finite values.
Results may differ from the reference program's by a relative error of at most 0.0143686.
Values are sent between devices in bfloat16 or wider.
A program may use at most 1 GiB of HBM per device.

```python
import jax
import jax.numpy as jnp
from jax import lax

IMAGES = 32
SEQ_LEN = 1024
WIDTH = 1152
HEADS = 16
HEAD_DIM = 72
MLP_DIM = 4304
LAYERS = 2
LN_EPS = 1e-6


def layer_norm(tokens, ln_gain, ln_shift):
    values = tokens.astype(jnp.float32)
    mean_val = jnp.mean(values, axis=-1, keepdims=True)
    centred = values - mean_val
    var_val = jnp.mean(centred * centred, axis=-1, keepdims=True)
    return (centred * lax.rsqrt(var_val + LN_EPS) * ln_gain + ln_shift).astype(jnp.bfloat16)


def one_head(head_inputs):
    q_head, k_head, v_head = head_inputs
    score_scale = q_head.shape[-1] ** -0.5
    scores = jnp.einsum('bqe,bke->bqk', q_head.astype(jnp.float32), k_head.astype(jnp.float32)) * score_scale
    row_peak = jnp.max(scores, axis=-1, keepdims=True)
    prob_vals = jnp.exp(scores - row_peak)
    row_total = jnp.sum(prob_vals, axis=-1, keepdims=True)
    mixed_vals = jnp.einsum('bqk,bke->bqe', prob_vals.astype(jnp.bfloat16).astype(jnp.float32), v_head.astype(jnp.float32))
    return (mixed_vals / row_total).astype(jnp.bfloat16)


def encoder_layer(hidden, layer_params):
    (ln1_gain, ln1_shift, w_qkv, b_qkv, w_out, b_out, ln2_gain, ln2_shift, w_up, b_up, w_down, b_down) = layer_params
    normed = layer_norm(hidden, ln1_gain, ln1_shift)
    qkv_all = jnp.einsum('bsd,dthe->bsthe', normed.astype(jnp.float32), w_qkv.astype(jnp.float32)) + b_qkv
    per_head = jnp.moveaxis(qkv_all.astype(jnp.bfloat16), 3, 0)
    heads_out = lax.map(one_head, (per_head[:, :, :, 0], per_head[:, :, :, 1], per_head[:, :, :, 2]))
    attn_proj = jnp.einsum('hbse,hed->bsd', heads_out.astype(jnp.float32), w_out.astype(jnp.float32)) + b_out
    mid_state = (hidden.astype(jnp.float32) + attn_proj).astype(jnp.bfloat16)
    normed_two = layer_norm(mid_state, ln2_gain, ln2_shift)
    up_proj = jnp.einsum('bsd,df->bsf', normed_two.astype(jnp.float32), w_up.astype(jnp.float32)) + b_up
    active = jax.nn.gelu(up_proj, approximate=True).astype(jnp.bfloat16)
    down_proj = jnp.einsum('bsf,fd->bsd', active.astype(jnp.float32), w_down.astype(jnp.float32)) + b_down
    return (mid_state.astype(jnp.float32) + down_proj).astype(jnp.bfloat16)


def setup_inputs(seed: int = 0, part: int = 0) -> dict:
    part_key = jax.random.fold_in(jax.random.key(seed), part)
    key_pattern, key_noise = jax.random.split(part_key, 2)
    period = SEQ_LEN // 8
    half_width = WIDTH // 2
    pattern = jax.random.normal(key_pattern, (IMAGES, period, half_width), jnp.float32)
    repeated = jnp.tile(pattern, (1, SEQ_LEN // period, 1))
    noise_part = jax.random.normal(key_noise, (IMAGES, SEQ_LEN, WIDTH - half_width), jnp.float32)
    image_tokens = jnp.concatenate([repeated, noise_part], axis=-1).astype(jnp.bfloat16)
    key_set = jax.random.split(jax.random.key(seed + 1), 14)
    row_scale = jnp.where(jnp.arange(WIDTH) < half_width, 1.0, 0.2)[:, None, None]
    head_shape = (LAYERS, WIDTH, HEADS, HEAD_DIM)
    w_query = 2.0 * WIDTH ** -0.5 * row_scale * jax.random.normal(key_set[0], head_shape, jnp.float32)
    w_key = w_query + 0.1 * WIDTH ** -0.5 * jax.random.normal(key_set[1], head_shape, jnp.float32)
    w_value = WIDTH ** -0.5 * jax.random.normal(key_set[2], head_shape, jnp.float32)
    w_qkv = jnp.stack([w_query, w_key, w_value], axis=2).astype(jnp.bfloat16)
    b_qkv = 0.3 * jax.random.normal(key_set[3], (LAYERS, 3, HEADS, HEAD_DIM), jnp.float32)
    w_out = (1.5 * WIDTH ** -0.5 * jax.random.normal(key_set[4], (LAYERS, HEADS, HEAD_DIM, WIDTH), jnp.float32)).astype(jnp.bfloat16)
    b_out = 0.3 * jax.random.normal(key_set[5], (LAYERS, WIDTH), jnp.float32)
    ln1_gain = 1.0 + 0.2 * jax.random.normal(key_set[6], (LAYERS, WIDTH), jnp.float32)
    ln1_shift = 0.3 * jax.random.normal(key_set[7], (LAYERS, WIDTH), jnp.float32)
    ln2_gain = 1.0 + 0.2 * jax.random.normal(key_set[8], (LAYERS, WIDTH), jnp.float32)
    ln2_shift = 0.3 * jax.random.normal(key_set[9], (LAYERS, WIDTH), jnp.float32)
    w_up = (WIDTH ** -0.5 * jax.random.normal(key_set[10], (LAYERS, WIDTH, MLP_DIM), jnp.float32)).astype(jnp.bfloat16)
    b_up = 0.3 * jax.random.normal(key_set[11], (LAYERS, MLP_DIM), jnp.float32)
    w_down = (0.5 * MLP_DIM ** -0.5 * jax.random.normal(key_set[12], (LAYERS, MLP_DIM, WIDTH), jnp.float32)).astype(jnp.bfloat16)
    b_down = 0.3 * jax.random.normal(key_set[13], (LAYERS, WIDTH), jnp.float32)
    return {'image_tokens': image_tokens, 'ln1_gain': ln1_gain, 'ln1_shift': ln1_shift, 'w_qkv': w_qkv, 'b_qkv': b_qkv, 'w_out': w_out, 'b_out': b_out, 'ln2_gain': ln2_gain, 'ln2_shift': ln2_shift, 'w_up': w_up, 'b_up': b_up, 'w_down': w_down, 'b_down': b_down}


def reference(image_tokens, ln1_gain, ln1_shift, w_qkv, b_qkv, w_out, b_out, ln2_gain, ln2_shift, w_up, b_up, w_down, b_down):
    stacked = (ln1_gain, ln1_shift, w_qkv, b_qkv, w_out, b_out, ln2_gain, ln2_shift, w_up, b_up, w_down, b_down)

    def layer_body(hidden, layer_params):
        return encoder_layer(hidden, layer_params), None

    return lax.scan(layer_body, image_tokens, stacked)[0]
```

```python
import functools
import math

import jax
import jax.numpy as jnp
from jax import lax
from jax.experimental import pallas as pl
from jax.experimental.pallas import tpu as pltpu
from jax.sharding import PartitionSpec as P

LN_EPS = 1e-6
LOG2E = math.log2(math.e)
VMEM_LIMIT = 60 * 1024 * 1024
BF16, F32 = jnp.bfloat16, jnp.float32


def layer_norm(tokens, gain, shift):
    values = tokens.astype(F32)
    mean_val = jnp.mean(values, axis=-1, keepdims=True)
    centred = values - mean_val
    var_val = jnp.mean(centred * centred, axis=-1, keepdims=True)
    return (centred * lax.rsqrt(var_val + LN_EPS) * gain + shift).astype(BF16)


def gelu_tanh(x):
    inner = x * (math.sqrt(2.0 / math.pi) + (math.sqrt(2.0 / math.pi) * 0.044715) * (x * x))
    half = 0.5 * x
    return half + half * jnp.tanh(inner)


def chunks(total, step):
    return [(start, min(step, total - start)) for start in range(0, total, step)]


def qkv_kernel(x_ref, gain_ref, shift_ref, w_ref, b_ref, o_ref, n_ref):
    parts, tile = x_ref.shape[0], x_ref.shape[2]
    per = n_ref.shape[1] // tile
    for sub in range(parts // per):
        for part in range(per):
            n_ref[sub, pl.ds(part * tile, tile), :] = layer_norm(x_ref[sub * per + part, 0], gain_ref[0], shift_ref[0])
    rows = n_ref.shape[1]
    for sub in range(parts // per):
        for start, size in chunks(w_ref.shape[2], 512):
            acc = jnp.dot(n_ref[sub], w_ref[0, :, pl.ds(start, size)], preferred_element_type=F32)
            o_ref[0, pl.ds(sub * rows, rows), pl.ds(start, size)] = (acc + b_ref[0, :, pl.ds(start, size)]).astype(BF16)


def attn_kernel(heads, head_dim, qkv_ref, x_ref, w_ref, b_ref, o_ref, vt_ref, ot_ref, of_ref, s_ref, p_ref):
    seq, width = qkv_ref.shape[1], heads * head_dim
    qb = s_ref.shape[2]
    scale = head_dim**-0.5 * LOG2E
    for start, size in chunks(width, 128):
        vt_ref[pl.ds(start, size), :] = qkv_ref[0, :, pl.ds(2 * width + start, size)].T

    lanes = lax.broadcasted_iota(jnp.int32, (1, 256), 1)
    pair_rows = 2 * head_dim

    def pair_body(pair, carry):
        units = [(hh, blk) for hh in range(2) for blk in range(seq // qb)]

        def scores(hh, blk, buf):
            first = (pair * 2 + hh) * head_dim
            off = pl.multiple_of(jnp.minimum(first // 128, width // 128 - 2) * 128, 128)
            mask = jnp.logical_and(lanes + off >= first, lanes + off < first + head_dim)
            k_win = qkv_ref[0, :, pl.ds(width + off, 256)]
            q_win = qkv_ref[0, pl.ds(blk * qb, qb), pl.ds(off, 256)]
            q_win = jnp.where(mask, q_win, jnp.zeros_like(q_win))
            s_ref[buf] = lax.dot_general(k_win, q_win, (((1,), (1,)), ((), ())), preferred_element_type=F32)

        def finish(hh, blk, buf):
            step = 64
            peak = s_ref[buf, pl.ds(0, 8), :]
            for r in range(8, seq, 8):
                peak = jnp.maximum(peak, s_ref[buf, pl.ds(r, 8), :])
            peak = jnp.max(peak, axis=0, keepdims=True)
            total = jnp.zeros((8, qb), F32)
            for r in range(0, seq, step):
                prob = jnp.exp2((s_ref[buf, pl.ds(r, step), :] - peak) * scale)
                p_ref[buf, pl.ds(r, step), :] = prob.astype(BF16)
                for g in range(0, step, 8):
                    total = total + prob[g : g + 8]
            total = jnp.sum(total, axis=0, keepdims=True)
            v_rows = pl.multiple_of(pair * pair_rows + 64 * hh, 16)
            mixed = jnp.dot(vt_ref[pl.ds(v_rows, 80), :], p_ref[buf], preferred_element_type=F32)
            mixed = mixed[8 * hh : 8 * hh + head_dim] * (1.0 / total)
            of_ref[pl.ds(hh * head_dim, head_dim), pl.ds(blk * qb, qb)] = mixed

        scores(*units[0], 0)
        for i, unit in enumerate(units):
            if i + 1 < len(units):
                scores(*units[i + 1], (i + 1) % 2)
            finish(*unit, i % 2)
        ot_ref[pl.ds(pl.multiple_of(pair * pair_rows, 16), pair_rows), :] = of_ref[...].astype(BF16)
        return carry

    lax.fori_loop(0, heads // 2, pair_body, 0)

    tile = x_ref.shape[2]
    for part in range(x_ref.shape[0]):
        o_part = ot_ref[:, pl.ds(part * tile, tile)].T
        acc = jnp.dot(o_part, w_ref[0], preferred_element_type=F32) + b_ref[0]
        o_ref[part, 0] = (x_ref[part, 0].astype(F32) + acc).astype(BF16)


def mlp_kernel(x_ref, gain_ref, shift_ref, wu_ref, bu_ref, wd_ref, bd_ref, o_ref, n_ref, a_ref):
    parts, tile = x_ref.shape[0], x_ref.shape[2]
    per = n_ref.shape[1] // tile
    for sub in range(parts // per):
        for part in range(per):
            n_ref[sub, pl.ds(part * tile, tile), :] = layer_norm(x_ref[sub * per + part, 0], gain_ref[0], shift_ref[0])
    for sub in range(parts // per):
        for start, size in chunks(wu_ref.shape[2], 512):
            acc = jnp.dot(n_ref[sub], wu_ref[0, :, pl.ds(start, size)], preferred_element_type=F32)
            a_ref[sub, :, pl.ds(start, size)] = gelu_tanh(acc + bu_ref[0, :, pl.ds(start, size)]).astype(BF16)
        acc = jnp.dot(a_ref[sub], wd_ref[0], preferred_element_type=F32) + bd_ref[0]
        for part in range(per):
            mid = x_ref[sub * per + part, 0].astype(F32)
            o_ref[sub * per + part, 0] = (mid + acc[part * tile : (part + 1) * tile]).astype(BF16)


def resident(shape, layer):
    return pl.BlockSpec((1,) + shape[1:], lambda *ids: (layer,) + (0,) * (len(shape) - 1), pipeline_mode=pl.Buffered(1))


def solution(mesh):
    token_spec = P('dp', 'sp', None)
    n = mesh.shape['sp']

    def device_step(image_tokens, ln1_gain, ln1_shift, w_qkv, b_qkv, w_out, b_out, ln2_gain, ln2_shift, w_up, b_up, w_down, b_down):
        images, tile, width = image_tokens.shape
        layers, _, _, heads, head_dim = w_qkv.shape
        mlp = w_up.shape[2]
        own, seq = images // n, n * tile
        row = lambda a: a.reshape(layers, 1, -1)
        w_qkv = w_qkv.reshape(layers, width, 3 * width)
        w_out = w_out.reshape(layers, width, width)
        ln1_gain, ln1_shift, b_qkv, b_out, ln2_gain, ln2_shift, b_up, b_down = map(
            row, (ln1_gain, ln1_shift, b_qkv, b_out, ln2_gain, ln2_shift, b_up, b_down)
        )
        tokens = image_tokens.shape[0] * tile
        params = pltpu.CompilerParams(vmem_limit_bytes=VMEM_LIMIT)
        half = n // 2
        h_shape = jax.ShapeDtypeStruct((n, own, tile, width), BF16)

        def qkv(h, layer):
            return pl.pallas_call(
                qkv_kernel,
                grid=(own, 2),
                out_shape=jax.ShapeDtypeStruct((own, seq, 3 * width), BF16),
                in_specs=[pl.BlockSpec((half, 1, tile, width), lambda i, j: (j, i, 0, 0))]
                + [resident(a.shape, layer) for a in (ln1_gain, ln1_shift, w_qkv, b_qkv)],
                out_specs=pl.BlockSpec((1, seq // 2, 3 * width), lambda i, j: (i, j, 0)),
                scratch_shapes=[pltpu.VMEM((2, seq // 4, width), BF16)],
                compiler_params=params,
                cost_estimate=pl.CostEstimate(flops=2 * tokens * width * 3 * width, bytes_accessed=2 * tokens * width * 4, transcendentals=0),
                name='qkv',
            )(h, ln1_gain, ln1_shift, w_qkv, b_qkv)

        def attend(qkv_all, h, layer):
            return pl.pallas_call(
                functools.partial(attn_kernel, heads, head_dim),
                grid=(own,),
                out_shape=h_shape,
                in_specs=[
                    pl.BlockSpec((1, seq, 3 * width), lambda i: (i, 0, 0)),
                    pl.BlockSpec((n, 1, tile, width), lambda i: (0, i, 0, 0)),
                    resident(w_out.shape, layer),
                    resident(b_out.shape, layer),
                ],
                out_specs=pl.BlockSpec((n, 1, tile, width), lambda i: (0, i, 0, 0)),
                scratch_shapes=[
                    pltpu.VMEM((width, seq), BF16),
                    pltpu.VMEM((width, seq), BF16),
                    pltpu.VMEM((2 * head_dim, seq), F32),
                    pltpu.VMEM((2, seq, 256), F32),
                    pltpu.VMEM((2, seq, 256), BF16),
                ],
                compiler_params=params,
                cost_estimate=pl.CostEstimate(
                    flops=4 * tokens * width * seq + 2 * tokens * width * width,
                    bytes_accessed=2 * tokens * width * 5,
                    transcendentals=tokens * heads * seq,
                ),
                name='attend',
            )(qkv_all, h, w_out, b_out)

        def mlp_layer(h, layer):
            return pl.pallas_call(
                mlp_kernel,
                grid=(own, 2),
                out_shape=h_shape,
                in_specs=[pl.BlockSpec((half, 1, tile, width), lambda i, j: (j, i, 0, 0))]
                + [resident(a.shape, layer) for a in (ln2_gain, ln2_shift, w_up, b_up, w_down, b_down)],
                out_specs=pl.BlockSpec((half, 1, tile, width), lambda i, j: (j, i, 0, 0)),
                scratch_shapes=[pltpu.VMEM((2, seq // 4, width), BF16), pltpu.VMEM((2, seq // 4, mlp), BF16)],
                compiler_params=params,
                cost_estimate=pl.CostEstimate(flops=4 * tokens * width * mlp, bytes_accessed=2 * tokens * width * 2, transcendentals=tokens * mlp),
                name='mlp',
            )(h, ln2_gain, ln2_shift, w_up, b_up, w_down, b_down)

        h = lax.all_to_all(image_tokens.reshape(n, own, tile, width), 'sp', 0, 0)
        for layer in range(layers):
            h = mlp_layer(attend(qkv(h, layer), h, layer), layer)
        h = lax.all_to_all(h, 'sp', 0, 0)
        return h.reshape(images, tile, width)

    return jax.shard_map(device_step, mesh=mesh, in_specs=(token_spec,) + (P(),) * 12, out_specs=token_spec, check_vma=False)
```

```python
import functools
import math

import jax
import jax.numpy as jnp
from jax import lax
from jax.experimental import pallas as pl
from jax.experimental.pallas import tpu as pltpu
from jax.sharding import PartitionSpec as P

LN_EPS = 1e-6
LOG2E = math.log2(math.e)
VMEM_LIMIT = 67_043_328
BF16, F32 = jnp.bfloat16, jnp.float32
MESH = pl.DeviceIdType.MESH
NT = (((1,), (1,)), ((), ()))


def layer_norm(tokens, gain, shift):
    values = tokens.astype(F32)
    mean_val = jnp.mean(values, axis=-1, keepdims=True)
    centred = values - mean_val
    var_val = jnp.mean(centred * centred, axis=-1, keepdims=True)
    return (centred * lax.rsqrt(var_val + LN_EPS) * gain + shift).astype(BF16)


def gelu_tanh(x):
    inner = x * (math.sqrt(2.0 / math.pi) + (math.sqrt(2.0 / math.pi) * 0.044715) * (x * x))
    half = 0.5 * x
    return half + half * jnp.tanh(inner)


def chunks(total, step):
    return [(start, min(step, total - start)) for start in range(0, total, step)]


def encoder_kernel(
    n, layers, heads, head_dim,
    x_hbm, g1_ref, s1_ref, wqkv_hbm, bqkv_ref, wout_hbm, bout_ref, g2_ref, s2_ref, wup_hbm, bup_ref, wdown_hbm, bdown_ref,
    out_hbm,
    h_ref, wqkv_ref, wout_ref, wup_ref, wdown_ref, qkv_ref, vt_ref, ot_ref, of_ref, s_ref, p_ref, n_ref, a_ref,
    w_sem, in_send, in_recv, out_send, out_recv,
):
    own, _, tile, width = h_ref.shape
    seq = n * tile
    mlp = wup_ref.shape[0]
    rows = n_ref.shape[0]
    per = rows // tile
    tiles = n // per
    qb = s_ref.shape[2]
    me = lax.axis_index('sp')
    dp = lax.axis_index('dp')

    def weight_copy(which, layer):
        src, dst = ((wqkv_hbm, wqkv_ref), (wout_hbm, wout_ref), (wup_hbm, wup_ref), (wdown_hbm, wdown_ref))[which]
        return pltpu.make_async_copy(src.at[layer], dst, w_sem.at[which])

    def send_in(image, peer):
        return pltpu.make_async_remote_copy(
            src_ref=x_hbm.at[peer * own + image], dst_ref=h_ref.at[image, me],
            send_sem=in_send.at[image, peer], recv_sem=in_recv.at[image, me], device_id=(dp, peer), device_id_type=MESH)

    def keep_in(image):
        return pltpu.make_async_copy(x_hbm.at[me * own + image], h_ref.at[image, me], in_recv.at[image, me])

    def send_out(image, peer):
        return pltpu.make_async_remote_copy(
            src_ref=h_ref.at[image, peer], dst_ref=out_hbm.at[me * own + image],
            send_sem=out_send.at[image, peer], recv_sem=out_recv.at[image, me], device_id=(dp, peer), device_id_type=MESH)

    def keep_out(image):
        return pltpu.make_async_copy(h_ref.at[image, me], out_hbm.at[me * own + image], out_recv.at[image, me])

    for which in range(4):
        weight_copy(which, 0).start()

    barrier = pltpu.get_barrier_semaphore()
    for k in range(1, n):
        pl.semaphore_signal(barrier, inc=1, device_id=(dp, lax.rem(me + k, n)), device_id_type=MESH)
    pl.semaphore_wait(barrier, n - 1)

    def start_in(image, carry):
        keep_in(image).start()

        def one(k, c):
            send_in(image, lax.rem(me + k, n)).start()
            return c

        return lax.fori_loop(1, n, one, carry)

    lax.fori_loop(0, own, start_in, 0)

    lanes = lax.broadcasted_iota(jnp.int32, (1, 256), 1)
    pair_rows = 2 * head_dim
    scale = head_dim**-0.5 * LOG2E
    last_window = width // 128 - 2
    pairs = heads // 2
    units = [(hh, blk) for hh in range(2) for blk in range(seq // qb)]

    def scores(pair, hh, blk, buf):
        first = (pair * 2 + hh) * head_dim
        off = pl.multiple_of(jnp.minimum(first // 128, last_window) * 128, 128)
        mask = jnp.logical_and(lanes + off >= first, lanes + off < first + head_dim)
        q_win = qkv_ref[pl.ds(blk * qb, qb), pl.ds(off, 256)]
        q_win = jnp.where(mask, q_win, jnp.zeros_like(q_win))
        for half in range(2):
            k_win = qkv_ref[pl.ds(half * (seq // 2), seq // 2), pl.ds(width + off, 256)]
            s_ref[buf, pl.ds(half * (seq // 2), seq // 2), :] = lax.dot_general(k_win, q_win, NT, preferred_element_type=F32)

    def finish(pair, hh, blk, buf):
        peak = jnp.max(s_ref[buf], axis=0, keepdims=True)
        total = jnp.zeros((1, qb), F32)
        for start, size in chunks(seq, 256):
            prob = jnp.exp2((s_ref[buf, pl.ds(start, size), :] - peak) * scale)
            p_ref[buf, pl.ds(start, size), :] = prob.astype(BF16)
            total = total + jnp.sum(prob, axis=0, keepdims=True)
        lane0 = jnp.minimum(pair * pair_rows // 128, last_window) * 128
        v_rows = pl.multiple_of(pair * pair_rows - lane0 + 64 * hh, 16)
        mixed = jnp.dot(vt_ref[pl.ds(v_rows, 80), :], p_ref[buf], preferred_element_type=F32)
        of_ref[pl.ds(hh * head_dim, head_dim), pl.ds(blk * qb, qb)] = mixed[8 * hh : 8 * hh + head_dim] * (1.0 / total)

    def pair_body(pair, carry):
        lane0 = pl.multiple_of(jnp.minimum(pair * pair_rows // 128, last_window) * 128, 128)
        vt_ref[...] = qkv_ref[:, pl.ds(2 * width + lane0, 256)].T
        following = jnp.minimum(pair + 1, pairs - 1)
        for i, (hh, blk) in enumerate(units):
            if i + 1 < len(units):
                scores(pair, *units[i + 1], (i + 1) % 2)
            else:
                scores(following, *units[0], (i + 1) % 2)
            finish(pair, hh, blk, i % 2)
        ot_ref[pl.ds(pl.multiple_of(pair * pair_rows, 16), pair_rows), :] = of_ref[...].astype(BF16)
        return carry

    def step(g, carry):
        layer, image = g // own, lax.rem(g, own)

        @pl.when(image == 0)
        def _():
            weight_copy(0, layer).wait()

        @pl.when(layer == 0)
        def _():
            keep_in(image).wait()
            for k in range(1, n):
                src = lax.rem(me + n - k, n)
                pltpu.make_async_remote_copy(
                    src_ref=x_hbm.at[image], dst_ref=h_ref.at[image, src], send_sem=in_send.at[image, src],
                    recv_sem=in_recv.at[image, src], device_id=(dp, src), device_id_type=MESH).wait_recv()

        def next_layer(which):
            @pl.when(jnp.logical_and(image == own - 1, layer < layers - 1))
            def _():
                weight_copy(which, layer + 1).start()

        def qkv_tile(t, c):
            tokens = h_ref[image, pl.ds(t * per, per)].reshape(rows, width)
            n_ref[...] = layer_norm(tokens, g1_ref[layer], s1_ref[layer])
            at = pl.ds(pl.multiple_of(t * rows, rows), rows)
            for start, size in chunks(3 * width, 512):
                acc = lax.dot_general(n_ref[...], wqkv_ref[pl.ds(start, size), :], NT, preferred_element_type=F32)
                qkv_ref[at, pl.ds(start, size)] = (acc + bqkv_ref[layer, :, pl.ds(start, size)]).astype(BF16)
            return c

        lax.fori_loop(0, tiles, qkv_tile, 0)
        next_layer(0)
        scores(0, *units[0], 0)
        lax.fori_loop(0, pairs, pair_body, 0)

        @pl.when(image == 0)
        def _():
            for which in range(1, 4):
                weight_copy(which, layer).wait()

        def mlp_tile(t, c):
            blocks = pl.ds(t * per, per)
            at = pl.ds(pl.multiple_of(t * rows, rows), rows)
            acc = jnp.dot(ot_ref[:, at].T, wout_ref[...], preferred_element_type=F32) + bout_ref[layer]
            mid = (h_ref[image, blocks].reshape(rows, width).astype(F32) + acc).astype(BF16)
            h_ref[image, blocks] = mid.reshape(per, tile, width)
            n_ref[...] = layer_norm(mid, g2_ref[layer], s2_ref[layer])
            for start, size in chunks(mlp, 512):
                acc = lax.dot_general(n_ref[...], wup_ref[pl.ds(start, size), :], NT, preferred_element_type=F32)
                a_ref[:, pl.ds(start, size)] = gelu_tanh(acc + bup_ref[layer, :, pl.ds(start, size)]).astype(BF16)
            acc = jnp.dot(a_ref[...], wdown_ref[...], preferred_element_type=F32) + bdown_ref[layer]
            new = h_ref[image, blocks].reshape(rows, width).astype(F32) + acc
            h_ref[image, blocks] = new.astype(BF16).reshape(per, tile, width)

            @pl.when(layer == layers - 1)
            def _():
                for part in range(per):
                    peer = t * per + part

                    @pl.when(peer == me)
                    def _():
                        keep_out(image).start()

                    @pl.when(peer != me)
                    def _():
                        send_out(image, peer).start()

            return c

        lax.fori_loop(0, tiles, mlp_tile, 0)
        for which in range(1, 4):
            next_layer(which)
        return carry

    lax.fori_loop(0, layers * own, step, 0)

    def drain(image, carry):
        keep_out(image).wait()
        for k in range(1, n):
            peer = lax.rem(me + k, n)
            send_in(image, peer).wait_send()
            send_out(image, peer).wait_send()
            pltpu.make_async_remote_copy(
                src_ref=h_ref.at[image, peer], dst_ref=out_hbm.at[peer * own + image], send_sem=out_send.at[image, peer],
                recv_sem=out_recv.at[image, peer], device_id=(dp, peer), device_id_type=MESH).wait_recv()
        return carry

    lax.fori_loop(0, own, drain, 0)


def solution(mesh):
    token_spec = P('dp', 'sp', None)
    n = mesh.shape['sp']

    def device_step(image_tokens, ln1_gain, ln1_shift, w_qkv, b_qkv, w_out, b_out, ln2_gain, ln2_shift, w_up, b_up, w_down, b_down):
        images, tile, width = image_tokens.shape
        layers, _, _, heads, head_dim = w_qkv.shape
        mlp = w_up.shape[2]
        own, seq = images // n, n * tile
        row = lambda a: a.reshape(layers, 1, -1)
        w_qkv = jnp.swapaxes(w_qkv.reshape(layers, width, 3 * width), 1, 2)
        w_up = jnp.swapaxes(w_up, 1, 2)
        w_out = w_out.reshape(layers, width, width)
        hbm = pl.BlockSpec(memory_space=pl.ANY)
        vmem = pl.BlockSpec(memory_space=pltpu.VMEM)
        rows = seq // 2
        return pl.pallas_call(
            functools.partial(encoder_kernel, n, layers, heads, head_dim),
            out_shape=jax.ShapeDtypeStruct(image_tokens.shape, BF16),
            in_specs=[hbm, vmem, vmem, hbm, vmem, hbm, vmem, vmem, vmem, hbm, vmem, hbm, vmem],
            out_specs=hbm,
            scratch_shapes=[
                pltpu.VMEM((own, n, tile, width), BF16),
                pltpu.VMEM((3 * width, width), BF16),
                pltpu.VMEM((width, width), BF16),
                pltpu.VMEM((mlp, width), BF16),
                pltpu.VMEM((mlp, width), BF16),
                pltpu.VMEM((seq, 3 * width), BF16),
                pltpu.VMEM((256, seq), BF16),
                pltpu.VMEM((width, seq), BF16),
                pltpu.VMEM((2 * head_dim, seq), F32),
                pltpu.VMEM((2, seq, 256), F32),
                pltpu.VMEM((2, seq, 256), BF16),
                pltpu.VMEM((rows, width), BF16),
                pltpu.VMEM((rows, mlp), BF16),
                pltpu.SemaphoreType.DMA((4,)),
                pltpu.SemaphoreType.DMA((own, n)),
                pltpu.SemaphoreType.DMA((own, n)),
                pltpu.SemaphoreType.DMA((own, n)),
                pltpu.SemaphoreType.DMA((own, n)),
            ],
            compiler_params=pltpu.CompilerParams(vmem_limit_bytes=VMEM_LIMIT, collective_id=0, has_side_effects=True),
            name='encoder',
        )(
            image_tokens, row(ln1_gain), row(ln1_shift), w_qkv, row(b_qkv), w_out, row(b_out),
            row(ln2_gain), row(ln2_shift), w_up, row(b_up), w_down, row(b_down),
        )

    return jax.shard_map(device_step, mesh=mesh, in_specs=(token_spec,) + (P(),) * 12, out_specs=token_spec, check_vma=False)
```

```python
import functools
import math

import jax
import jax.numpy as jnp
from jax import lax
from jax.experimental import pallas as pl
from jax.experimental.pallas import tpu as pltpu
from jax.sharding import PartitionSpec as P

LN_EPS = 1e-6
LOG2E = math.log2(math.e)
VMEM_LIMIT = 67_043_328
BF16, F32 = jnp.bfloat16, jnp.float32
MESH = pl.DeviceIdType.MESH
NT = (((1,), (1,)), ((), ()))
RELATION = (0, 1, 2, 4, 3, 5, 6, 7)
QKV_CHUNK, UP_CHUNK, DOWN_CHUNK = 512, 512, 1152


def layer_norm(tokens, gain, shift):
    values = tokens.astype(F32)
    mean_val = jnp.mean(values, axis=-1, keepdims=True)
    centred = values - mean_val
    var_val = jnp.mean(centred * centred, axis=-1, keepdims=True)
    return (centred * lax.rsqrt(var_val + LN_EPS) * gain + shift).astype(BF16)


def gelu_tanh(x):
    inner = x * (math.sqrt(2.0 / math.pi) + (math.sqrt(2.0 / math.pi) * 0.044715) * (x * x))
    half = 0.5 * x
    return half + half * jnp.tanh(inner)


def chunks(total, step):
    return [(start, min(step, total - start)) for start in range(0, total, step)]


def encoder_kernel(
    n, layers, heads, head_dim,
    x_hbm, g1_ref, s1_ref, wqkv_hbm, bqkv_ref, wout_hbm, bout_ref, g2_ref, s2_ref, wup_hbm, bup_ref, wdown_hbm, bdown_ref,
    out_hbm,
    h_ref, wqkv_ref, wout_ref, wup_ref, wdown_ref, qkv_ref, vt_ref, ot_ref, of_ref, s_ref, p_ref, n_ref, a_ref,
    w_sem, in_send, in_recv, out_send, out_recv,
):
    own, _, tile, width = h_ref.shape
    seq = n * tile
    mlp = wup_ref.shape[0]
    rows = a_ref.shape[0]
    per = rows // tile
    tiles = n // per
    qb = s_ref.shape[2]
    me = lax.axis_index('sp')
    dp = lax.axis_index('dp')

    def weight_copy(which, layer):
        src, dst = ((wqkv_hbm, wqkv_ref), (wout_hbm, wout_ref), (wup_hbm, wup_ref), (wdown_hbm, wdown_ref))[which]
        return pltpu.make_async_copy(src.at[layer], dst, w_sem.at[which])

    def peer_of(slot):
        rel = RELATION[slot]
        return sum((me // bit + rel // bit) % 2 * bit for bit in (1, 2, 4))

    def send_in(image, slot):
        peer = peer_of(slot)
        return pltpu.make_async_remote_copy(
            src_ref=x_hbm.at[peer * own + image], dst_ref=h_ref.at[image, slot],
            send_sem=in_send.at[image, slot], recv_sem=in_recv.at[image, slot], device_id=(dp, peer), device_id_type=MESH)

    def keep_in(image):
        return pltpu.make_async_copy(x_hbm.at[me * own + image], h_ref.at[image, 0], in_recv.at[image, 0])

    def send_out(image, slot):
        return pltpu.make_async_remote_copy(
            src_ref=h_ref.at[image, slot], dst_ref=out_hbm.at[me * own + image],
            send_sem=out_send.at[image, slot], recv_sem=out_recv.at[image, slot], device_id=(dp, peer_of(slot)), device_id_type=MESH)

    def keep_out(image):
        return pltpu.make_async_copy(h_ref.at[image, 0], out_hbm.at[me * own + image], out_recv.at[image, 0])

    for which in range(4):
        weight_copy(which, 0).start()

    barrier = pltpu.get_barrier_semaphore()
    for k in range(1, n):
        pl.semaphore_signal(barrier, inc=1, device_id=(dp, peer_of(k)), device_id_type=MESH)
    pl.semaphore_wait(barrier, n - 1)

    def start_in(image, carry):
        keep_in(image).start()
        for slot in range(1, n):
            send_in(image, slot).start()
        return carry

    lax.fori_loop(0, own, start_in, 0)

    lanes = lax.broadcasted_iota(jnp.int32, (1, 256), 1)
    scale = head_dim**-0.5 * LOG2E
    pair_rows = 2 * head_dim
    last_window = width // 128 - 2
    pairs = heads // 2
    units = [(hh, blk) for hh in range(2) for blk in range(seq // qb)]

    def scores(pair, hh, blk, buf):
        first = (pair * 2 + hh) * head_dim
        off = pl.multiple_of(jnp.minimum(first // 128, last_window) * 128, 128)
        mask = jnp.logical_and(lanes + off >= first, lanes + off < first + head_dim)
        q_win = qkv_ref[pl.ds(blk * qb, qb), pl.ds(off, 256)]
        q_win = jnp.where(mask, q_win, jnp.zeros_like(q_win))
        for half in range(2):
            k_win = qkv_ref[pl.ds(half * (seq // 2), seq // 2), pl.ds(width + off, 256)]
            s_ref[buf, pl.ds(half * (seq // 2), seq // 2), :] = lax.dot_general(k_win, q_win, NT, preferred_element_type=F32)

    def finish(pair, hh, blk, buf):
        peak = jnp.max(s_ref[buf], axis=0, keepdims=True)
        total = jnp.zeros((1, qb), F32)
        for start, size in chunks(seq, 256):
            prob = jnp.exp2(s_ref[buf, pl.ds(start, size), :] - peak)
            p_ref[buf, pl.ds(start, size), :] = prob.astype(BF16)
            total = total + jnp.sum(prob, axis=0, keepdims=True)
        lane0 = jnp.minimum(pair * pair_rows // 128, last_window) * 128
        v_rows = pl.multiple_of(pair * pair_rows - lane0 + 64 * hh, 16)
        mixed = jnp.dot(vt_ref[pl.ds(v_rows, 80), :], p_ref[buf], preferred_element_type=F32)
        of_ref[pl.ds(hh * head_dim, head_dim), pl.ds(blk * qb, qb)] = mixed[8 * hh : 8 * hh + head_dim] * (1.0 / total)

    def pair_body(pair, carry):
        lane0 = pl.multiple_of(jnp.minimum(pair * pair_rows // 128, last_window) * 128, 128)
        vt_ref[...] = qkv_ref[:, pl.ds(2 * width + lane0, 256)].T
        following = jnp.minimum(pair + 1, pairs - 1)
        for i, (hh, blk) in enumerate(units):
            if i + 1 < len(units):
                scores(pair, *units[i + 1], (i + 1) % 2)
            else:
                scores(following, *units[0], (i + 1) % 2)
            finish(pair, hh, blk, i % 2)
        ot_ref[pl.ds(pl.multiple_of(pair * pair_rows, 16), pair_rows), :] = of_ref[...].astype(BF16)
        return carry

    def step(g, carry):
        layer, image = g // own, lax.rem(g, own)

        @pl.when(image == 0)
        def _():
            weight_copy(0, layer).wait()

        def next_layer(which):
            @pl.when(jnp.logical_and(image == own - 1, layer < layers - 1))
            def _():
                weight_copy(which, layer + 1).start()

        def arrive(first, last):
            @pl.when(layer == 0)
            def _():
                for slot in range(first, last):
                    if slot:
                        send_in(image, slot).wait_recv()
                    else:
                        keep_in(image).wait()

        def row_of(ref, start, size):
            return ref[pl.ds(layer, 1), :][:, start : start + size]

        def qkv_columns(n_at, rows_at, start, size):
            acc = lax.dot_general(n_ref[n_at, :], wqkv_ref[pl.ds(start, size), :], NT, preferred_element_type=F32)
            acc = acc + row_of(bqkv_ref, start, size)
            if start < width:
                cols = start + lax.broadcasted_iota(jnp.int32, (1, size), 1)
                acc = acc * jnp.where(cols < width, scale, 1.0)
            qkv_ref[rows_at, pl.ds(start, size)] = acc.astype(BF16)

        def qkv_tile(t, c):
            @pl.when(layer == 0)
            def _():
                @pl.when(t == 0)
                def _():
                    arrive(0, per)

                @pl.when(t == 1)
                def _():
                    arrive(per, n)

            half = rows // 2
            for sub in range(2):
                tokens = h_ref[image, pl.ds(t * per + sub * per // 2, per // 2)].reshape(half, width)
                n_ref[pl.ds(sub * half, half), :] = layer_norm(tokens, row_of(g1_ref, 0, width), row_of(s1_ref, 0, width))
                qkv_columns(pl.ds(sub * half, half), pl.ds(pl.multiple_of(t * rows + sub * half, half), half), 0, 512)
            for start, size in chunks(3 * width - 512, QKV_CHUNK):
                qkv_columns(pl.ds(0, rows), pl.ds(pl.multiple_of(t * rows, rows), rows), 512 + start, size)
            return c

        lax.fori_loop(0, tiles, qkv_tile, 0)
        next_layer(0)
        scores(0, *units[0], 0)
        lax.fori_loop(0, pairs, pair_body, 0)

        @pl.when(image == 0)
        def _():
            for which in range(1, 4):
                weight_copy(which, layer).wait()

        def out_tile(t):
            blocks = pl.ds(t * per, per)
            acc = jnp.dot(ot_ref[:, pl.ds(t * rows, rows)].T, wout_ref[...], preferred_element_type=F32) + row_of(bout_ref, 0, width)
            mid = (h_ref[image, blocks].reshape(rows, width).astype(F32) + acc).astype(BF16)
            h_ref[image, blocks] = mid.reshape(per, tile, width)
            n_ref[pl.ds(t * rows, rows), :] = layer_norm(mid, row_of(g2_ref, 0, width), row_of(s2_ref, 0, width))

        def mlp_tile(t):
            blocks = pl.ds(t * per, per)
            for start, size in chunks(mlp, UP_CHUNK):
                acc = lax.dot_general(n_ref[pl.ds(t * rows, rows), :], wup_ref[pl.ds(start, size), :], NT, preferred_element_type=F32)
                a_ref[:, pl.ds(start, size)] = gelu_tanh(acc + row_of(bup_ref, start, size)).astype(BF16)
            for start, size in chunks(width, DOWN_CHUNK):
                acc = jnp.dot(a_ref[...], wdown_ref[:, pl.ds(start, size)], preferred_element_type=F32) + row_of(bdown_ref, start, size)
                new = h_ref[image, blocks, :, pl.ds(start, size)].reshape(rows, size).astype(F32) + acc
                h_ref[image, blocks, :, pl.ds(start, size)] = new.astype(BF16).reshape(per, tile, size)

            @pl.when(layer == layers - 1)
            def _():
                for slot in range(t * per, (t + 1) * per):
                    if slot:
                        send_out(image, slot).start()
                    else:
                        keep_out(image).start()

        for t in reversed(range(tiles)):
            out_tile(t)
        for t in reversed(range(tiles)):
            mlp_tile(t)
        for which in range(1, 4):
            next_layer(which)
        return carry

    lax.fori_loop(0, layers * own, step, 0)

    def drain(image, carry):
        keep_out(image).wait()
        for slot in range(1, n):
            send_in(image, slot).wait_send()
            send_out(image, slot).wait()
        return carry

    lax.fori_loop(0, own, drain, 0)


def solution(mesh):
    token_spec = P('dp', 'sp', None)
    n = mesh.shape['sp']

    def device_step(image_tokens, ln1_gain, ln1_shift, w_qkv, b_qkv, w_out, b_out, ln2_gain, ln2_shift, w_up, b_up, w_down, b_down):
        images, tile, width = image_tokens.shape
        layers, _, _, heads, head_dim = w_qkv.shape
        mlp = w_up.shape[2]
        own, seq = images // n, n * tile
        w_qkv = jnp.swapaxes(w_qkv.reshape(layers, width, 3 * width), 1, 2)
        w_up = jnp.swapaxes(w_up, 1, 2)
        w_out = w_out.reshape(layers, width, width)
        hbm = pl.BlockSpec(memory_space=pl.ANY)
        vmem = pl.BlockSpec(memory_space=pltpu.VMEM)
        rows = seq // 2
        return pl.pallas_call(
            functools.partial(encoder_kernel, n, layers, heads, head_dim),
            out_shape=jax.ShapeDtypeStruct(image_tokens.shape, BF16),
            in_specs=[hbm, vmem, vmem, hbm, vmem, hbm, vmem, vmem, vmem, hbm, vmem, hbm, vmem],
            out_specs=hbm,
            scratch_shapes=[
                pltpu.VMEM((own, n, tile, width), BF16),
                pltpu.VMEM((3 * width, width), BF16),
                pltpu.VMEM((width, width), BF16),
                pltpu.VMEM((mlp, width), BF16),
                pltpu.VMEM((mlp, width), BF16),
                pltpu.VMEM((seq, 3 * width), BF16),
                pltpu.VMEM((256, seq), BF16),
                pltpu.VMEM((width, seq), BF16),
                pltpu.VMEM((2 * head_dim, seq), F32),
                pltpu.VMEM((2, seq, 256), F32),
                pltpu.VMEM((2, seq, 256), BF16),
                pltpu.VMEM((seq, width), BF16),
                pltpu.VMEM((rows, mlp), BF16),
                pltpu.SemaphoreType.DMA((4,)),
                pltpu.SemaphoreType.DMA((own, n)),
                pltpu.SemaphoreType.DMA((own, n)),
                pltpu.SemaphoreType.DMA((own, n)),
                pltpu.SemaphoreType.DMA((own, n)),
            ],
            compiler_params=pltpu.CompilerParams(vmem_limit_bytes=VMEM_LIMIT, collective_id=0, has_side_effects=True),
            name='encoder',
        )(
            image_tokens, ln1_gain, ln1_shift, w_qkv, b_qkv.reshape(layers, 3 * width), w_out, b_out,
            ln2_gain, ln2_shift, w_up, b_up, w_down, b_down,
        )

    return jax.shard_map(device_step, mesh=mesh, in_specs=(token_spec,) + (P(),) * 12, out_specs=token_spec, check_vma=False)
```

```python
import functools
import math

import jax
import jax.numpy as jnp
from jax import lax
from jax.experimental import pallas as pl
from jax.experimental.pallas import tpu as pltpu
from jax.sharding import PartitionSpec as P

LN_EPS = 1e-6
LOG2E = math.log2(math.e)
VMEM_LIMIT = 67_043_328
BF16, F32 = jnp.bfloat16, jnp.float32
MESH = pl.DeviceIdType.MESH
NT = (((1,), (1,)), ((), ()))
RELATION = (0, 1, 2, 4, 3, 5, 6, 7)
QKV_CHUNK, UP_CHUNK, DOWN_CHUNK = 512, 512, 1152
PAIRS, BUFFERS, AHEAD = 1, 4, 2


def layer_norm(tokens, gain, shift):
    values = tokens.astype(F32)
    mean_val = jnp.mean(values, axis=-1, keepdims=True)
    centred = values - mean_val
    var_val = jnp.mean(centred * centred, axis=-1, keepdims=True)
    return (centred * lax.rsqrt(var_val + LN_EPS) * gain + shift).astype(BF16)


def gelu_tanh(x):
    inner = x * (math.sqrt(2.0 / math.pi) + (math.sqrt(2.0 / math.pi) * 0.044715) * (x * x))
    half = 0.5 * x
    return half + half * jnp.tanh(inner)


def chunks(total, step):
    return [(start, min(step, total - start)) for start in range(0, total, step)]


def to_planes(ref, start, rows_at, values):
    for lane, size in chunks(values.shape[1], 128):
        ref[(start + lane) // 128, rows_at, pl.ds(0, size)] = values[:, lane : lane + size]


def from_planes(ref, rows_at, total):
    return jnp.concatenate([ref[start // 128, rows_at, pl.ds(0, size)] for start, size in chunks(total, 128)], axis=1)


def encoder_kernel(
    n, layers, heads, head_dim,
    x_hbm, g1_ref, s1_ref, wqkv_hbm, bqkv_ref, wout_hbm, bout_ref, g2_ref, s2_ref, wup_hbm, bup_ref, wdown_hbm, bdown_ref,
    out_hbm,
    h_ref, wqkv_ref, wout_ref, wup_ref, wdown_ref, qkv_ref, vt_ref, ot_ref, of_ref, s_ref, a_ref,
    w_sem, in_send, in_recv, out_send, out_recv,
):
    own, _, tile, width = h_ref.shape
    seq = n * tile
    mlp = wup_ref.shape[0]
    rows = a_ref.shape[1]
    per = rows // tile
    tiles = n // per
    qb = s_ref.shape[2]
    me = lax.axis_index('sp')
    dp = lax.axis_index('dp')

    def weight_copy(which, layer):
        src, dst = ((wqkv_hbm, wqkv_ref), (wout_hbm, wout_ref), (wup_hbm, wup_ref), (wdown_hbm, wdown_ref))[which]
        return pltpu.make_async_copy(src.at[layer], dst, w_sem.at[which])

    def peer_of(slot):
        rel = RELATION[slot]
        return sum((me // bit + rel // bit) % 2 * bit for bit in (1, 2, 4))

    def send_in(image, slot):
        peer = peer_of(slot)
        return pltpu.make_async_remote_copy(
            src_ref=x_hbm.at[peer * own + image], dst_ref=h_ref.at[image, slot],
            send_sem=in_send.at[image, slot], recv_sem=in_recv.at[image, slot], device_id=(dp, peer), device_id_type=MESH)

    def keep_in(image):
        return pltpu.make_async_copy(x_hbm.at[me * own + image], h_ref.at[image, 0], in_recv.at[image, 0])

    def send_out(image, slot):
        return pltpu.make_async_remote_copy(
            src_ref=h_ref.at[image, slot], dst_ref=out_hbm.at[me * own + image],
            send_sem=out_send.at[image, slot], recv_sem=out_recv.at[image, slot], device_id=(dp, peer_of(slot)), device_id_type=MESH)

    def keep_out(image):
        return pltpu.make_async_copy(h_ref.at[image, 0], out_hbm.at[me * own + image], out_recv.at[image, 0])

    for which in range(4):
        weight_copy(which, 0).start()

    barrier = pltpu.get_barrier_semaphore()
    for k in range(1, n):
        pl.semaphore_signal(barrier, inc=1, device_id=(dp, peer_of(k)), device_id_type=MESH)
    pl.semaphore_wait(barrier, n - 1)

    def start_in(image, carry):
        keep_in(image).start()
        for slot in range(1, n):
            send_in(image, slot).start()
        return carry

    lax.fori_loop(0, own, start_in, 0)

    lanes = lax.broadcasted_iota(jnp.int32, (1, 256), 1)
    scale = head_dim**-0.5 * LOG2E
    pair_rows = 2 * head_dim
    last_window = width // 128 - 2
    pairs = heads // 2
    planes = width // 128

    def window(first):
        return jnp.minimum(first // 128, last_window)

    def two_planes(plane, start, size):
        return jnp.concatenate([qkv_ref[plane + i, pl.ds(start, size), :] for i in range(2)], axis=1)

    def scores(pair, hh, blk, buf):
        first = (pair * 2 + hh) * head_dim
        plane = window(first)
        mask = jnp.logical_and(lanes + plane * 128 >= first, lanes + plane * 128 < first + head_dim)
        q_win = two_planes(plane, blk * qb, qb)
        q_win = jnp.where(mask, q_win, jnp.zeros_like(q_win))
        for half in range(2):
            k_win = two_planes(planes + plane, half * (seq // 2), seq // 2)
            s_ref[buf, pl.ds(half * (seq // 2), seq // 2), :] = lax.dot_general(k_win, q_win, NT, preferred_element_type=F32)

    def finish(pair, e, hh, blk, buf):
        peak = jnp.max(s_ref[buf], axis=0, keepdims=True)
        total = jnp.zeros((1, qb), F32)
        probs = []
        for start, size in chunks(seq, 256):
            prob = jnp.exp2(s_ref[buf, pl.ds(start, size), :] - peak)
            probs.append(prob.astype(BF16))
            total = total + jnp.sum(prob, axis=0, keepdims=True)
        first = pair * pair_rows
        v_rows = pl.multiple_of(first - window(first) * 128 + 64 * hh, 16)
        values = jnp.concatenate([vt_ref[e, part, pl.ds(v_rows, 80), :] for part in range(seq // 128)], axis=1)
        mixed = jnp.dot(values, jnp.concatenate(probs, axis=0), preferred_element_type=F32)
        of_ref[e, pl.ds(hh * head_dim, head_dim), pl.ds(blk * qb, qb)] = mixed[8 * hh : 8 * hh + head_dim] * (1.0 / total)

    units = [(e, hh, blk) for e in range(PAIRS) for hh in range(2) for blk in range(seq // qb)]

    def pairs_body(it, carry):
        following = jnp.minimum((it + 1) * PAIRS, pairs - 1)
        for e in range(PAIRS):
            plane = 2 * planes + window((it * PAIRS + e) * pair_rows)
            for part in range(seq // 128):
                vt_ref[e, part] = two_planes(plane, part * 128, 128).T
        for i, (e, hh, blk) in enumerate(units):
            ahead = i + AHEAD
            e1, hh1, blk1 = units[ahead % len(units)]
            scores(it * PAIRS + e1 if ahead < len(units) else following, hh1, blk1, ahead % BUFFERS)
            finish(it * PAIRS + e, e, hh, blk, i % BUFFERS)
            if (hh, blk) == (1, seq // qb - 1):
                at = pl.multiple_of((it * PAIRS + e) * pair_rows, 16)
                ot_ref[pl.ds(at, pair_rows), :] = of_ref[e].astype(BF16)
        return carry

    def step(g, carry):
        layer, image = g // own, lax.rem(g, own)

        @pl.when(image == 0)
        def _():
            weight_copy(0, layer).wait()

        def next_layer(which):
            @pl.when(jnp.logical_and(image == own - 1, layer < layers - 1))
            def _():
                weight_copy(which, layer + 1).start()

        def arrive(first, last):
            @pl.when(layer == 0)
            def _():
                for slot in range(first, last):
                    if slot:
                        send_in(image, slot).wait_recv()
                    else:
                        keep_in(image).wait()

        def row_of(ref, start, size):
            return ref[pl.ds(layer, 1), :][:, start : start + size]

        def qkv_columns(n_at, rows_at, start, size):
            acc = lax.dot_general(from_planes(a_ref, n_at, width), wqkv_ref[pl.ds(start, size), :], NT, preferred_element_type=F32)
            acc = acc + row_of(bqkv_ref, start, size)
            if start < width:
                cols = start + lax.broadcasted_iota(jnp.int32, (1, size), 1)
                acc = acc * jnp.where(cols < width, scale, 1.0)
            to_planes(qkv_ref, start, rows_at, acc.astype(BF16))

        def qkv_tile(t, c):
            @pl.when(layer == 0)
            def _():
                @pl.when(t == 0)
                def _():
                    arrive(0, per)

                @pl.when(t == 1)
                def _():
                    arrive(per, n)

            half = rows // 2
            for sub in range(2):
                tokens = h_ref[image, pl.ds(t * per + sub * per // 2, per // 2)].reshape(half, width)
                normed = layer_norm(tokens, row_of(g1_ref, 0, width), row_of(s1_ref, 0, width))
                to_planes(a_ref, 0, pl.ds(sub * half, half), normed)
                qkv_columns(pl.ds(sub * half, half), pl.ds(pl.multiple_of(t * rows + sub * half, half), half), 0, 512)
            for start, size in chunks(3 * width - 512, QKV_CHUNK):
                qkv_columns(pl.ds(0, rows), pl.ds(pl.multiple_of(t * rows, rows), rows), 512 + start, size)
            return c

        lax.fori_loop(0, tiles, qkv_tile, 0)
        next_layer(0)
        for i, (_, hh, blk) in enumerate(units[:AHEAD]):
            scores(0, hh, blk, i)
        lax.fori_loop(0, pairs // PAIRS, pairs_body, 0)

        @pl.when(image == 0)
        def _():
            for which in range(1, 4):
                weight_copy(which, layer).wait()

        def out_tile(t):
            blocks = pl.ds(t * per, per)
            acc = jnp.dot(ot_ref[:, pl.ds(t * rows, rows)].T, wout_ref[...], preferred_element_type=F32) + row_of(bout_ref, 0, width)
            mid = (h_ref[image, blocks].reshape(rows, width).astype(F32) + acc).astype(BF16)
            h_ref[image, blocks] = mid.reshape(per, tile, width)
            to_planes(qkv_ref, 0, pl.ds(t * rows, rows), layer_norm(mid, row_of(g2_ref, 0, width), row_of(s2_ref, 0, width)))

        def mlp_tile(t):
            blocks = pl.ds(t * per, per)
            for start, size in chunks(mlp, UP_CHUNK):
                acc = lax.dot_general(from_planes(qkv_ref, pl.ds(t * rows, rows), width), wup_ref[pl.ds(start, size), :], NT, preferred_element_type=F32)
                to_planes(a_ref, start, pl.ds(0, rows), gelu_tanh(acc + row_of(bup_ref, start, size)).astype(BF16))
            for start, size in chunks(width, DOWN_CHUNK):
                acc = jnp.dot(from_planes(a_ref, pl.ds(0, rows), mlp), wdown_ref[:, pl.ds(start, size)], preferred_element_type=F32) + row_of(bdown_ref, start, size)
                new = h_ref[image, blocks, :, pl.ds(start, size)].reshape(rows, size).astype(F32) + acc
                h_ref[image, blocks, :, pl.ds(start, size)] = new.astype(BF16).reshape(per, tile, size)

            @pl.when(layer == layers - 1)
            def _():
                for slot in range(t * per, (t + 1) * per):
                    if slot:
                        send_out(image, slot).start()
                    else:
                        keep_out(image).start()

        for t in reversed(range(tiles)):
            out_tile(t)
        for t in reversed(range(tiles)):
            mlp_tile(t)
        for which in range(1, 4):
            next_layer(which)
        return carry

    lax.fori_loop(0, layers * own, step, 0)

    def drain(image, carry):
        keep_out(image).wait()
        for slot in range(1, n):
            send_in(image, slot).wait_send()
            send_out(image, slot).wait()
        return carry

    lax.fori_loop(0, own, drain, 0)


def solution(mesh):
    token_spec = P('dp', 'sp', None)
    n = mesh.shape['sp']

    def device_step(image_tokens, ln1_gain, ln1_shift, w_qkv, b_qkv, w_out, b_out, ln2_gain, ln2_shift, w_up, b_up, w_down, b_down):
        images, tile, width = image_tokens.shape
        layers, _, _, heads, head_dim = w_qkv.shape
        mlp = w_up.shape[2]
        own, seq = images // n, n * tile
        w_qkv = jnp.swapaxes(w_qkv.reshape(layers, width, 3 * width), 1, 2)
        w_up = jnp.swapaxes(w_up, 1, 2)
        w_out = w_out.reshape(layers, width, width)
        hbm = pl.BlockSpec(memory_space=pl.ANY)
        vmem = pl.BlockSpec(memory_space=pltpu.VMEM)
        rows = seq // 2
        return pl.pallas_call(
            functools.partial(encoder_kernel, n, layers, heads, head_dim),
            out_shape=jax.ShapeDtypeStruct(image_tokens.shape, BF16),
            in_specs=[hbm, vmem, vmem, hbm, vmem, hbm, vmem, vmem, vmem, hbm, vmem, hbm, vmem],
            out_specs=hbm,
            scratch_shapes=[
                pltpu.VMEM((own, n, tile, width), BF16),
                pltpu.VMEM((3 * width, width), BF16),
                pltpu.VMEM((width, width), BF16),
                pltpu.VMEM((mlp, width), BF16),
                pltpu.VMEM((mlp, width), BF16),
                pltpu.VMEM((3 * width // 128, seq, 128), BF16),
                pltpu.VMEM((PAIRS, seq // 128, 256, 128), BF16),
                pltpu.VMEM((width, seq), BF16),
                pltpu.VMEM((PAIRS, 2 * head_dim, seq), F32),
                pltpu.VMEM((BUFFERS, seq, 256), F32),
                pltpu.VMEM((pl.cdiv(mlp, 128), rows, 128), BF16),
                pltpu.SemaphoreType.DMA((4,)),
                pltpu.SemaphoreType.DMA((own, n)),
                pltpu.SemaphoreType.DMA((own, n)),
                pltpu.SemaphoreType.DMA((own, n)),
                pltpu.SemaphoreType.DMA((own, n)),
            ],
            compiler_params=pltpu.CompilerParams(vmem_limit_bytes=VMEM_LIMIT, collective_id=0, has_side_effects=True),
            name='encoder',
        )(
            image_tokens, ln1_gain, ln1_shift, w_qkv, b_qkv.reshape(layers, 3 * width), w_out, b_out,
            ln2_gain, ln2_shift, w_up, b_up, w_down, b_down,
        )

    return jax.shard_map(device_step, mesh=mesh, in_specs=(token_spec,) + (P(),) * 12, out_specs=token_spec, check_vma=False)
```

```python
import functools
import math

import jax
import jax.numpy as jnp
from jax import lax
from jax.experimental import pallas as pl
from jax.experimental.pallas import tpu as pltpu
from jax.sharding import PartitionSpec as P

LN_EPS = 1e-6
LOG2E = math.log2(math.e)
VMEM_LIMIT = 67_043_328
BF16, F32 = jnp.bfloat16, jnp.float32
MESH = pl.DeviceIdType.MESH
NT = (((1,), (1,)), ((), ()))
RELATION = (0, 1, 2, 4, 3, 5, 6, 7)
QKV_CHUNK, UP_CHUNK, DOWN_CHUNK = 512, 512, 1152
PAIRS, BUFFERS, AHEAD = 2, 4, 2


def layer_norm(tokens, gain, shift):
    values = tokens.astype(F32)
    mean_val = jnp.mean(values, axis=-1, keepdims=True)
    centred = values - mean_val
    var_val = jnp.mean(centred * centred, axis=-1, keepdims=True)
    return (centred * lax.rsqrt(var_val + LN_EPS) * gain + shift).astype(BF16)


def gelu_tanh(x):
    inner = x * (math.sqrt(2.0 / math.pi) + (math.sqrt(2.0 / math.pi) * 0.044715) * (x * x))
    half = 0.5 * x
    return half + half * jnp.tanh(inner)


def chunks(total, step):
    return [(start, min(step, total - start)) for start in range(0, total, step)]


def to_planes(ref, start, rows_at, values):
    for lane, size in chunks(values.shape[1], 128):
        ref[(start + lane) // 128, rows_at, pl.ds(0, size)] = values[:, lane : lane + size]


def from_planes(ref, rows_at, total):
    return jnp.concatenate([ref[start // 128, rows_at, pl.ds(0, size)] for start, size in chunks(total, 128)], axis=1)


def encoder_kernel(
    n, layers, heads, head_dim,
    x_hbm, g1_ref, s1_ref, wqkv_hbm, bqkv_ref, wout_hbm, bout_ref, g2_ref, s2_ref, wup_hbm, bup_ref, wdown_hbm, bdown_ref,
    out_hbm,
    h_ref, wqkv_ref, wout_ref, wup_ref, wdown_ref, qk_ref, vt_ref, ot_ref, of_ref, s_ref, a_ref,
    w_sem, in_send, in_recv, out_send, out_recv,
):
    own, _, tile, width = h_ref.shape
    seq = n * tile
    mlp = wup_ref.shape[0]
    rows = a_ref.shape[1]
    per = rows // tile
    tiles = n // per
    qb = s_ref.shape[2]
    me = lax.axis_index('sp')
    dp = lax.axis_index('dp')

    def weight_copy(which, layer):
        src, dst = ((wqkv_hbm, wqkv_ref), (wout_hbm, wout_ref), (wup_hbm, wup_ref), (wdown_hbm, wdown_ref))[which]
        return pltpu.make_async_copy(src.at[layer], dst, w_sem.at[which])

    def peer_of(slot):
        rel = RELATION[slot]
        return sum((me // bit + rel // bit) % 2 * bit for bit in (1, 2, 4))

    def send_in(image, slot):
        peer = peer_of(slot)
        return pltpu.make_async_remote_copy(
            src_ref=x_hbm.at[peer * own + image], dst_ref=h_ref.at[image, slot],
            send_sem=in_send.at[image, slot], recv_sem=in_recv.at[image, slot], device_id=(dp, peer), device_id_type=MESH)

    def keep_in(image):
        return pltpu.make_async_copy(x_hbm.at[me * own + image], h_ref.at[image, 0], in_recv.at[image, 0])

    def send_out(image, slot):
        return pltpu.make_async_remote_copy(
            src_ref=h_ref.at[image, slot], dst_ref=out_hbm.at[me * own + image],
            send_sem=out_send.at[image, slot], recv_sem=out_recv.at[image, slot], device_id=(dp, peer_of(slot)), device_id_type=MESH)

    def keep_out(image):
        return pltpu.make_async_copy(h_ref.at[image, 0], out_hbm.at[me * own + image], out_recv.at[image, 0])

    for which in range(4):
        weight_copy(which, 0).start()

    barrier = pltpu.get_barrier_semaphore()
    for k in range(1, n):
        pl.semaphore_signal(barrier, inc=1, device_id=(dp, peer_of(k)), device_id_type=MESH)
    pl.semaphore_wait(barrier, n - 1)

    def start_in(image, carry):
        keep_in(image).start()
        for slot in range(1, n):
            send_in(image, slot).start()
        return carry

    lax.fori_loop(0, own, start_in, 0)

    lanes = lax.broadcasted_iota(jnp.int32, (1, 256), 1)
    scale = head_dim**-0.5 * LOG2E
    pair_rows = 2 * head_dim
    last_window = width // 128 - 2
    pairs = heads // 2
    planes = width // 128

    def window(first):
        return jnp.minimum(first // 128, last_window)

    def two_planes(plane, start, size):
        return jnp.concatenate([qk_ref[plane + i, pl.ds(start, size), :] for i in range(2)], axis=1)

    def scores(pair, hh, blk, buf):
        first = (pair * 2 + hh) * head_dim
        plane = window(first)
        mask = jnp.logical_and(lanes + plane * 128 >= first, lanes + plane * 128 < first + head_dim)
        q_win = two_planes(plane, blk * qb, qb)
        q_win = jnp.where(mask, q_win, jnp.zeros_like(q_win))
        for half in range(2):
            k_win = two_planes(planes + plane, half * (seq // 2), seq // 2)
            s_ref[buf, pl.ds(half * (seq // 2), seq // 2), :] = lax.dot_general(k_win, q_win, NT, preferred_element_type=F32)

    def softmax(buf):
        peak = jnp.max(s_ref[buf], axis=0, keepdims=True)
        total = jnp.zeros((1, qb), F32)
        probs = []
        for start, size in chunks(seq, 256):
            prob = jnp.exp2(s_ref[buf, pl.ds(start, size), :] - peak)
            probs.append(prob.astype(BF16))
            total = total + jnp.sum(prob, axis=0, keepdims=True)
        return jnp.concatenate(probs, axis=0), total

    def mix(pair, e, hh, blk, probs, total):
        v_rows = pl.ds(pl.multiple_of(pair * pair_rows + 64 * hh, 16), 80)
        values = jnp.concatenate([vt_ref[part, v_rows, :] for part in range(seq // 128)], axis=1)
        mixed = jnp.dot(values, probs, preferred_element_type=F32)
        of_ref[e, pl.ds(hh * head_dim, head_dim), pl.ds(blk * qb, qb)] = mixed[8 * hh : 8 * hh + head_dim] * (1.0 / total)

    units = [(e, hh, blk) for e in range(PAIRS) for hh in range(2) for blk in range(seq // qb)]

    def pairs_body(it, carry):
        following = jnp.minimum((it + 1) * PAIRS, pairs - 1)
        waiting = None
        for i, (e, hh, blk) in enumerate(units):
            ahead = i + AHEAD
            e1, hh1, blk1 = units[ahead % len(units)]
            scores(it * PAIRS + e1 if ahead < len(units) else following, hh1, blk1, ahead % BUFFERS)
            done = softmax(i % BUFFERS)
            if waiting:
                mix(*waiting)
            waiting = (it * PAIRS + e, e, hh, blk, *done)
        mix(*waiting)
        for e in range(PAIRS):
            at = pl.multiple_of((it * PAIRS + e) * pair_rows, 16)
            ot_ref[pl.ds(at, pair_rows), :] = of_ref[e].astype(BF16)
        return carry

    def step(g, carry):
        layer, image = g // own, lax.rem(g, own)

        @pl.when(image == 0)
        def _():
            weight_copy(0, layer).wait()

        def next_layer(which):
            @pl.when(jnp.logical_and(image == own - 1, layer < layers - 1))
            def _():
                weight_copy(which, layer + 1).start()

        def arrive(first, last):
            @pl.when(layer == 0)
            def _():
                for slot in range(first, last):
                    if slot:
                        send_in(image, slot).wait_recv()
                    else:
                        keep_in(image).wait()

        def row_of(ref, start, size):
            return ref[pl.ds(layer, 1), :][:, start : start + size]

        def qk_columns(n_at, rows_at, start, size):
            acc = lax.dot_general(from_planes(a_ref, n_at, width), wqkv_ref[pl.ds(start, size), :], NT, preferred_element_type=F32)
            acc = acc + row_of(bqkv_ref, start, size)
            if start < width:
                cols = start + lax.broadcasted_iota(jnp.int32, (1, size), 1)
                acc = acc * jnp.where(cols < width, scale, 1.0)
            to_planes(qk_ref, start, rows_at, acc.astype(BF16))

        def v_columns(t, start, size):
            first = 2 * width + start
            acc = lax.dot_general(from_planes(a_ref, pl.ds(0, rows), width), wqkv_ref[pl.ds(first, size), :], NT, preferred_element_type=F32)
            flipped = (acc + row_of(bqkv_ref, first, size)).astype(BF16).T
            for part in range(per):
                vt_ref[t * per + part, pl.ds(start, size), :] = flipped[:, part * tile : (part + 1) * tile]

        def qkv_tile(t, c):
            @pl.when(layer == 0)
            def _():
                @pl.when(t == 0)
                def _():
                    arrive(0, per)

                @pl.when(t == 1)
                def _():
                    arrive(per, n)

            half = rows // 2
            for sub in range(2):
                tokens = h_ref[image, pl.ds(t * per + sub * per // 2, per // 2)].reshape(half, width)
                normed = layer_norm(tokens, row_of(g1_ref, 0, width), row_of(s1_ref, 0, width))
                to_planes(a_ref, 0, pl.ds(sub * half, half), normed)
                qk_columns(pl.ds(sub * half, half), pl.ds(pl.multiple_of(t * rows + sub * half, half), half), 0, 512)
            for start, size in chunks(width, QKV_CHUNK):
                v_columns(t, start, size)
            for start, size in chunks(2 * width - 512, QKV_CHUNK):
                qk_columns(pl.ds(0, rows), pl.ds(pl.multiple_of(t * rows, rows), rows), 512 + start, size)
            return c

        lax.fori_loop(0, tiles, qkv_tile, 0)
        next_layer(0)
        for i, (_, hh, blk) in enumerate(units[:AHEAD]):
            scores(0, hh, blk, i)
        lax.fori_loop(0, pairs // PAIRS, pairs_body, 0)

        @pl.when(image == 0)
        def _():
            for which in range(1, 4):
                weight_copy(which, layer).wait()

        def out_tile(t):
            blocks = pl.ds(t * per, per)
            acc = jnp.dot(ot_ref[:, pl.ds(t * rows, rows)].T, wout_ref[...], preferred_element_type=F32) + row_of(bout_ref, 0, width)
            mid = (h_ref[image, blocks].reshape(rows, width).astype(F32) + acc).astype(BF16)
            h_ref[image, blocks] = mid.reshape(per, tile, width)
            to_planes(qk_ref, 0, pl.ds(t * rows, rows), layer_norm(mid, row_of(g2_ref, 0, width), row_of(s2_ref, 0, width)))

        def mlp_tile(t):
            blocks = pl.ds(t * per, per)
            for start, size in chunks(mlp, UP_CHUNK):
                acc = lax.dot_general(from_planes(qk_ref, pl.ds(t * rows, rows), width), wup_ref[pl.ds(start, size), :], NT, preferred_element_type=F32)
                to_planes(a_ref, start, pl.ds(0, rows), gelu_tanh(acc + row_of(bup_ref, start, size)).astype(BF16))
            for start, size in chunks(width, DOWN_CHUNK):
                acc = jnp.dot(from_planes(a_ref, pl.ds(0, rows), mlp), wdown_ref[:, pl.ds(start, size)], preferred_element_type=F32) + row_of(bdown_ref, start, size)
                new = h_ref[image, blocks, :, pl.ds(start, size)].reshape(rows, size).astype(F32) + acc
                h_ref[image, blocks, :, pl.ds(start, size)] = new.astype(BF16).reshape(per, tile, size)

            @pl.when(layer == layers - 1)
            def _():
                for slot in range(t * per, (t + 1) * per):
                    if slot:
                        send_out(image, slot).start()
                    else:
                        keep_out(image).start()

        for t in reversed(range(tiles)):
            out_tile(t)
        for t in reversed(range(tiles)):
            mlp_tile(t)
        for which in range(1, 4):
            next_layer(which)
        return carry

    lax.fori_loop(0, layers * own, step, 0)

    def drain(image, carry):
        keep_out(image).wait()
        for slot in range(1, n):
            send_in(image, slot).wait_send()
            send_out(image, slot).wait()
        return carry

    lax.fori_loop(0, own, drain, 0)


def solution(mesh):
    token_spec = P('dp', 'sp', None)
    n = mesh.shape['sp']

    def device_step(image_tokens, ln1_gain, ln1_shift, w_qkv, b_qkv, w_out, b_out, ln2_gain, ln2_shift, w_up, b_up, w_down, b_down):
        images, tile, width = image_tokens.shape
        layers, _, _, heads, head_dim = w_qkv.shape
        mlp = w_up.shape[2]
        own, seq = images // n, n * tile
        w_qkv = jnp.swapaxes(w_qkv.reshape(layers, width, 3 * width), 1, 2)
        w_up = jnp.swapaxes(w_up, 1, 2)
        w_out = w_out.reshape(layers, width, width)
        hbm = pl.BlockSpec(memory_space=pl.ANY)
        vmem = pl.BlockSpec(memory_space=pltpu.VMEM)
        rows = seq // 2
        return pl.pallas_call(
            functools.partial(encoder_kernel, n, layers, heads, head_dim),
            out_shape=jax.ShapeDtypeStruct(image_tokens.shape, BF16),
            in_specs=[hbm, vmem, vmem, hbm, vmem, hbm, vmem, vmem, vmem, hbm, vmem, hbm, vmem],
            out_specs=hbm,
            scratch_shapes=[
                pltpu.VMEM((own, n, tile, width), BF16),
                pltpu.VMEM((3 * width, width), BF16),
                pltpu.VMEM((width, width), BF16),
                pltpu.VMEM((mlp, width), BF16),
                pltpu.VMEM((mlp, width), BF16),
                pltpu.VMEM((2 * width // 128, seq, 128), BF16),
                pltpu.VMEM((seq // 128, width, 128), BF16),
                pltpu.VMEM((width, seq), BF16),
                pltpu.VMEM((PAIRS, 2 * head_dim, seq), F32),
                pltpu.VMEM((BUFFERS, seq, 256), F32),
                pltpu.VMEM((pl.cdiv(mlp, 128), rows, 128), BF16),
                pltpu.SemaphoreType.DMA((4,)),
                pltpu.SemaphoreType.DMA((own, n)),
                pltpu.SemaphoreType.DMA((own, n)),
                pltpu.SemaphoreType.DMA((own, n)),
                pltpu.SemaphoreType.DMA((own, n)),
            ],
            compiler_params=pltpu.CompilerParams(vmem_limit_bytes=VMEM_LIMIT, collective_id=0, has_side_effects=True),
            name='encoder',
        )(
            image_tokens, ln1_gain, ln1_shift, w_qkv, b_qkv.reshape(layers, 3 * width), w_out, b_out,
            ln2_gain, ln2_shift, w_up, b_up, w_down, b_down,
        )

    return jax.shard_map(device_step, mesh=mesh, in_specs=(token_spec,) + (P(),) * 12, out_specs=token_spec, check_vma=False)
```

```python
import functools
import math

import jax
import jax.numpy as jnp
from jax import lax
from jax.experimental import pallas as pl
from jax.experimental.pallas import tpu as pltpu
from jax.sharding import PartitionSpec as P

LN_EPS = 1e-6
LOG2E = math.log2(math.e)
VMEM_LIMIT = 67_043_328
BF16, F32 = jnp.bfloat16, jnp.float32
MESH = pl.DeviceIdType.MESH
NT = (((1,), (1,)), ((), ()))
RELATION = (0, 1, 2, 4, 3, 5, 6, 7)
QKV_CHUNK, UP_CHUNK, DOWN_CHUNK = 512, 512, 1152
PAIRS, BUFFERS, AHEAD = 2, 4, 2


def layer_norm(tokens, gain, shift):
    values = tokens.astype(F32)
    mean_val = jnp.mean(values, axis=-1, keepdims=True)
    centred = values - mean_val
    var_val = jnp.mean(centred * centred, axis=-1, keepdims=True)
    return (centred * lax.rsqrt(var_val + LN_EPS) * gain + shift).astype(BF16)


def gelu_tanh(x):
    inner = x * (math.sqrt(2.0 / math.pi) + (math.sqrt(2.0 / math.pi) * 0.044715) * (x * x))
    half = 0.5 * x
    return half + half * jnp.tanh(inner)


def chunks(total, step):
    return [(start, min(step, total - start)) for start in range(0, total, step)]


def to_planes(ref, start, rows_at, values):
    for lane, size in chunks(values.shape[1], 128):
        ref[(start + lane) // 128, rows_at, pl.ds(0, size)] = values[:, lane : lane + size]


def from_planes(ref, rows_at, total):
    return jnp.concatenate([ref[start // 128, rows_at, pl.ds(0, size)] for start, size in chunks(total, 128)], axis=1)


def encoder_kernel(
    n, layers, heads, head_dim,
    x_hbm, g1_ref, s1_ref, wqkv_hbm, bqkv_ref, wout_hbm, bout_ref, g2_ref, s2_ref, wup_hbm, bup_ref, wdown_hbm, bdown_ref,
    out_hbm,
    h_ref, wqkv_ref, wout_ref, wup_ref, wdown_ref, qk_ref, vt_ref, ot_ref, of_ref, s_ref, a_ref,
    w_sem, in_send, in_recv, out_send, out_recv,
):
    own, _, tile, width = h_ref.shape
    seq = n * tile
    mlp = wup_ref.shape[0]
    rows = a_ref.shape[1]
    per = rows // tile
    tiles = n // per
    qb = s_ref.shape[2]
    me = lax.axis_index('sp')
    dp = lax.axis_index('dp')

    def weight_copy(which, layer):
        src, dst = ((wqkv_hbm, wqkv_ref), (wout_hbm, wout_ref), (wup_hbm, wup_ref), (wdown_hbm, wdown_ref))[which]
        return pltpu.make_async_copy(src.at[layer], dst, w_sem.at[which])

    def peer_of(slot):
        rel = RELATION[slot]
        return sum((me // bit + rel // bit) % 2 * bit for bit in (1, 2, 4))

    def send_in(image, slot):
        peer = peer_of(slot)
        return pltpu.make_async_remote_copy(
            src_ref=x_hbm.at[peer * own + image], dst_ref=h_ref.at[image, slot],
            send_sem=in_send.at[image, slot], recv_sem=in_recv.at[image, slot], device_id=(dp, peer), device_id_type=MESH)

    def keep_in(image):
        return pltpu.make_async_copy(x_hbm.at[me * own + image], h_ref.at[image, 0], in_recv.at[image, 0])

    def send_out(image, slot):
        return pltpu.make_async_remote_copy(
            src_ref=h_ref.at[image, slot], dst_ref=out_hbm.at[me * own + image],
            send_sem=out_send.at[image, slot], recv_sem=out_recv.at[image, slot], device_id=(dp, peer_of(slot)), device_id_type=MESH)

    def keep_out(image):
        return pltpu.make_async_copy(h_ref.at[image, 0], out_hbm.at[me * own + image], out_recv.at[image, 0])

    weight_copy(0, 0).start()

    barrier = pltpu.get_barrier_semaphore()
    for k in range(1, n):
        pl.semaphore_signal(barrier, inc=1, device_id=(dp, peer_of(k)), device_id_type=MESH)
    pl.semaphore_wait(barrier, n - 1)

    def start_in(image):
        keep_in(image).start()
        for slot in range(1, n):
            send_in(image, slot).start()

    start_in(0)
    for which in range(1, 4):
        weight_copy(which, 0).start()
    for image in range(1, own):
        start_in(image)

    lanes = lax.broadcasted_iota(jnp.int32, (1, 256), 1)
    scale = head_dim**-0.5 * LOG2E
    pair_rows = 2 * head_dim
    last_window = width // 128 - 2
    pairs = heads // 2
    planes = width // 128

    def window(first):
        return jnp.minimum(first // 128, last_window)

    def two_planes(plane, start, size):
        return jnp.concatenate([qk_ref[plane + i, pl.ds(start, size), :] for i in range(2)], axis=1)

    def scores(pair, hh, blk, buf):
        first = (pair * 2 + hh) * head_dim
        plane = window(first)
        mask = jnp.logical_and(lanes + plane * 128 >= first, lanes + plane * 128 < first + head_dim)
        q_win = two_planes(plane, blk * qb, qb)
        q_win = jnp.where(mask, q_win, jnp.zeros_like(q_win))
        for half in range(2):
            k_win = two_planes(planes + plane, half * (seq // 2), seq // 2)
            s_ref[buf, pl.ds(half * (seq // 2), seq // 2), :] = lax.dot_general(k_win, q_win, NT, preferred_element_type=F32)

    def softmax(buf):
        peak = jnp.max(s_ref[buf], axis=0, keepdims=True)
        total = jnp.zeros((1, qb), F32)
        probs = []
        for start, size in chunks(seq, 256):
            prob = jnp.exp2(s_ref[buf, pl.ds(start, size), :] - peak)
            probs.append(prob.astype(BF16))
            total = total + jnp.sum(prob, axis=0, keepdims=True)
        return jnp.concatenate(probs, axis=0), total

    def mix(pair, e, hh, blk, probs, total):
        v_rows = pl.ds(pl.multiple_of(pair * pair_rows + 64 * hh, 16), 80)
        values = jnp.concatenate([vt_ref[part, v_rows, :] for part in range(seq // 128)], axis=1)
        mixed = jnp.dot(values, probs, preferred_element_type=F32)
        of_ref[e, pl.ds(hh * head_dim, head_dim), pl.ds(blk * qb, qb)] = mixed[8 * hh : 8 * hh + head_dim] * (1.0 / total)

    units = [(e, hh, blk) for e in range(PAIRS) for hh in range(2) for blk in range(seq // qb)]

    def pairs_body(it, carry):
        following = jnp.minimum((it + 1) * PAIRS, pairs - 1)
        waiting = None
        for i, (e, hh, blk) in enumerate(units):
            ahead = i + AHEAD
            e1, hh1, blk1 = units[ahead % len(units)]
            scores(it * PAIRS + e1 if ahead < len(units) else following, hh1, blk1, ahead % BUFFERS)
            done = softmax(i % BUFFERS)
            if waiting:
                mix(*waiting)
            waiting = (it * PAIRS + e, e, hh, blk, *done)
        mix(*waiting)
        for e in range(PAIRS):
            at = pl.multiple_of((it * PAIRS + e) * pair_rows, 16)
            ot_ref[pl.ds(at, pair_rows), :] = of_ref[e].astype(BF16)
        return carry

    def step(g, carry):
        layer, image = g // own, lax.rem(g, own)

        @pl.when(image == 0)
        def _():
            weight_copy(0, layer).wait()

        def next_layer(which):
            @pl.when(jnp.logical_and(image == own - 1, layer < layers - 1))
            def _():
                weight_copy(which, layer + 1).start()

        def arrive(first, last):
            @pl.when(layer == 0)
            def _():
                for slot in range(first, last):
                    if slot:
                        send_in(image, slot).wait_recv()
                    else:
                        keep_in(image).wait()

        def row_of(ref, start, size):
            return ref[pl.ds(layer, 1), :][:, start : start + size]

        def qk_columns(n_at, rows_at, start, size):
            acc = lax.dot_general(from_planes(a_ref, n_at, width), wqkv_ref[pl.ds(start, size), :], NT, preferred_element_type=F32)
            acc = acc + row_of(bqkv_ref, start, size)
            if start < width:
                cols = start + lax.broadcasted_iota(jnp.int32, (1, size), 1)
                acc = acc * jnp.where(cols < width, scale, 1.0)
            to_planes(qk_ref, start, rows_at, acc.astype(BF16))

        def v_columns(t, start, size):
            first = 2 * width + start
            acc = lax.dot_general(from_planes(a_ref, pl.ds(0, rows), width), wqkv_ref[pl.ds(first, size), :], NT, preferred_element_type=F32)
            flipped = (acc + row_of(bqkv_ref, first, size)).astype(BF16).T
            for part in range(per):
                vt_ref[t * per + part, pl.ds(start, size), :] = flipped[:, part * tile : (part + 1) * tile]

        def qkv_tile(t, c):
            @pl.when(layer == 0)
            def _():
                @pl.when(t == 0)
                def _():
                    arrive(0, per)

                @pl.when(t == 1)
                def _():
                    arrive(per, n)

            half = rows // 2
            for sub in range(2):
                tokens = h_ref[image, pl.ds(t * per + sub * per // 2, per // 2)].reshape(half, width)
                normed = layer_norm(tokens, row_of(g1_ref, 0, width), row_of(s1_ref, 0, width))
                to_planes(a_ref, 0, pl.ds(sub * half, half), normed)
                qk_columns(pl.ds(sub * half, half), pl.ds(pl.multiple_of(t * rows + sub * half, half), half), 0, 512)
            for start, size in chunks(width, QKV_CHUNK):
                v_columns(t, start, size)
            for start, size in chunks(2 * width - 512, QKV_CHUNK):
                qk_columns(pl.ds(0, rows), pl.ds(pl.multiple_of(t * rows, rows), rows), 512 + start, size)
            return c

        lax.fori_loop(0, tiles, qkv_tile, 0)
        next_layer(0)
        for i, (_, hh, blk) in enumerate(units[:AHEAD]):
            scores(0, hh, blk, i)
        lax.fori_loop(0, pairs // PAIRS, pairs_body, 0)

        @pl.when(image == 0)
        def _():
            for which in range(1, 4):
                weight_copy(which, layer).wait()

        def out_tile(t):
            blocks = pl.ds(t * per, per)
            acc = jnp.dot(ot_ref[:, pl.ds(t * rows, rows)].T, wout_ref[...], preferred_element_type=F32) + row_of(bout_ref, 0, width)
            mid = (h_ref[image, blocks].reshape(rows, width).astype(F32) + acc).astype(BF16)
            h_ref[image, blocks] = mid.reshape(per, tile, width)
            to_planes(qk_ref, 0, pl.ds(t * rows, rows), layer_norm(mid, row_of(g2_ref, 0, width), row_of(s2_ref, 0, width)))

        def mlp_tile(t):
            blocks = pl.ds(t * per, per)
            for start, size in chunks(mlp, UP_CHUNK):
                acc = lax.dot_general(from_planes(qk_ref, pl.ds(t * rows, rows), width), wup_ref[pl.ds(start, size), :], NT, preferred_element_type=F32)
                to_planes(a_ref, start, pl.ds(0, rows), gelu_tanh(acc + row_of(bup_ref, start, size)).astype(BF16))
            for start, size in chunks(width, DOWN_CHUNK):
                acc = jnp.dot(from_planes(a_ref, pl.ds(0, rows), mlp), wdown_ref[:, pl.ds(start, size)], preferred_element_type=F32) + row_of(bdown_ref, start, size)
                new = h_ref[image, blocks, :, pl.ds(start, size)].reshape(rows, size).astype(F32) + acc
                h_ref[image, blocks, :, pl.ds(start, size)] = new.astype(BF16).reshape(per, tile, size)

            @pl.when(layer == layers - 1)
            def _():
                for slot in range(t * per, (t + 1) * per):
                    if slot:
                        send_out(image, slot).start()
                    else:
                        keep_out(image).start()

        for t in reversed(range(tiles)):
            out_tile(t)
        for t in reversed(range(tiles)):
            mlp_tile(t)
        for which in range(1, 4):
            next_layer(which)
        return carry

    lax.fori_loop(0, layers * own, step, 0)

    def drain(image, carry):
        keep_out(image).wait()
        for slot in range(1, n):
            send_in(image, slot).wait_send()
            send_out(image, slot).wait()
        return carry

    lax.fori_loop(0, own, drain, 0)


def solution(mesh):
    token_spec = P('dp', 'sp', None)
    n = mesh.shape['sp']

    def device_step(image_tokens, ln1_gain, ln1_shift, w_qkv, b_qkv, w_out, b_out, ln2_gain, ln2_shift, w_up, b_up, w_down, b_down):
        images, tile, width = image_tokens.shape
        layers, _, _, heads, head_dim = w_qkv.shape
        mlp = w_up.shape[2]
        own, seq = images // n, n * tile
        w_qkv = jnp.swapaxes(w_qkv.reshape(layers, width, 3 * width), 1, 2)
        w_up = jnp.swapaxes(w_up, 1, 2)
        w_out = w_out.reshape(layers, width, width)
        hbm = pl.BlockSpec(memory_space=pl.ANY)
        vmem = pl.BlockSpec(memory_space=pltpu.VMEM)
        rows = seq // 2
        return pl.pallas_call(
            functools.partial(encoder_kernel, n, layers, heads, head_dim),
            out_shape=jax.ShapeDtypeStruct(image_tokens.shape, BF16),
            in_specs=[hbm, vmem, vmem, hbm, vmem, hbm, vmem, vmem, vmem, hbm, vmem, hbm, vmem],
            out_specs=hbm,
            scratch_shapes=[
                pltpu.VMEM((own, n, tile, width), BF16),
                pltpu.VMEM((3 * width, width), BF16),
                pltpu.VMEM((width, width), BF16),
                pltpu.VMEM((mlp, width), BF16),
                pltpu.VMEM((mlp, width), BF16),
                pltpu.VMEM((2 * width // 128, seq, 128), BF16),
                pltpu.VMEM((seq // 128, width, 128), BF16),
                pltpu.VMEM((width, seq), BF16),
                pltpu.VMEM((PAIRS, 2 * head_dim, seq), F32),
                pltpu.VMEM((BUFFERS, seq, 256), F32),
                pltpu.VMEM((pl.cdiv(mlp, 128), rows, 128), BF16),
                pltpu.SemaphoreType.DMA((4,)),
                pltpu.SemaphoreType.DMA((own, n)),
                pltpu.SemaphoreType.DMA((own, n)),
                pltpu.SemaphoreType.DMA((own, n)),
                pltpu.SemaphoreType.DMA((own, n)),
            ],
            compiler_params=pltpu.CompilerParams(vmem_limit_bytes=VMEM_LIMIT, collective_id=0, has_side_effects=True),
            name='encoder',
        )(
            image_tokens, ln1_gain, ln1_shift, w_qkv, b_qkv.reshape(layers, 3 * width), w_out, b_out,
            ln2_gain, ln2_shift, w_up, b_up, w_down, b_down,
        )

    return jax.shard_map(device_step, mesh=mesh, in_specs=(token_spec,) + (P(),) * 12, out_specs=token_spec, check_vma=False)
```

```python
import functools
import math

import jax
import jax.numpy as jnp
from jax import lax
from jax.experimental import pallas as pl
from jax.experimental.pallas import tpu as pltpu
from jax.sharding import PartitionSpec as P

LN_EPS = 1e-6
LOG2E = math.log2(math.e)
VMEM_LIMIT = 67_043_328
BF16, F32 = jnp.bfloat16, jnp.float32
MESH = pl.DeviceIdType.MESH
NT = (((1,), (1,)), ((), ()))
RELATION = (0, 1, 2, 4, 3, 5, 6, 7)
QKV_CHUNK, UP_CHUNK, DOWN_CHUNK = 512, 512, 1152
PAIRS, BUFFERS, AHEAD = 2, 4, 2


def layer_norm(tokens, gain, shift):
    values = tokens.astype(F32)
    mean_val = jnp.mean(values, axis=-1, keepdims=True)
    centred = values - mean_val
    var_val = jnp.mean(centred * centred, axis=-1, keepdims=True)
    return (centred * lax.rsqrt(var_val + LN_EPS) * gain + shift).astype(BF16)


def gelu_tanh(x):
    inner = x * (math.sqrt(2.0 / math.pi) + (math.sqrt(2.0 / math.pi) * 0.044715) * (x * x))
    half = 0.5 * x
    return half + half * jnp.tanh(inner)


def chunks(total, step):
    return [(start, min(step, total - start)) for start in range(0, total, step)]


def to_planes(ref, start, rows_at, values):
    for lane, size in chunks(values.shape[1], 128):
        ref[(start + lane) // 128, rows_at, pl.ds(0, size)] = values[:, lane : lane + size]


def from_planes(ref, rows_at, total):
    return jnp.concatenate([ref[start // 128, rows_at, pl.ds(0, size)] for start, size in chunks(total, 128)], axis=1)


def encoder_kernel(
    n, layers, heads, head_dim,
    x_hbm, g1_ref, s1_ref, wqkv_hbm, bias_ref, wout_hbm, bout_ref, g2_ref, s2_ref, wup_hbm, bup_ref, wdown_hbm, bdown_ref,
    out_hbm,
    h_ref, wqkv_ref, wout_ref, wup_ref, wdown_ref, qk_ref, vt_ref, ot_ref, of_ref, s_ref, a_ref, bqkv_ref,
    w_sem, in_send, in_recv, out_send, out_recv,
):
    own, _, tile, width = h_ref.shape
    seq = n * tile
    mlp = wup_ref.shape[0]
    rows = a_ref.shape[1]
    per = rows // tile
    tiles = n // per
    qb = s_ref.shape[2]
    me = lax.axis_index('sp')
    dp = lax.axis_index('dp')

    def weight_copy(which, layer):
        src, dst = ((wqkv_hbm, wqkv_ref), (wout_hbm, wout_ref), (wup_hbm, wup_ref), (wdown_hbm, wdown_ref))[which]
        return pltpu.make_async_copy(src.at[layer], dst, w_sem.at[which])

    def peer_of(slot):
        rel = RELATION[slot]
        return sum((me // bit + rel // bit) % 2 * bit for bit in (1, 2, 4))

    def send_in(image, slot):
        peer = peer_of(slot)
        return pltpu.make_async_remote_copy(
            src_ref=x_hbm.at[peer * own + image], dst_ref=h_ref.at[image, slot],
            send_sem=in_send.at[image, slot], recv_sem=in_recv.at[image, slot], device_id=(dp, peer), device_id_type=MESH)

    def keep_in(image):
        return pltpu.make_async_copy(x_hbm.at[me * own + image], h_ref.at[image, 0], in_recv.at[image, 0])

    def send_out(image, slot):
        return pltpu.make_async_remote_copy(
            src_ref=h_ref.at[image, slot], dst_ref=out_hbm.at[me * own + image],
            send_sem=out_send.at[image, slot], recv_sem=out_recv.at[image, slot], device_id=(dp, peer_of(slot)), device_id_type=MESH)

    def keep_out(image):
        return pltpu.make_async_copy(h_ref.at[image, 0], out_hbm.at[me * own + image], out_recv.at[image, 0])

    weight_copy(0, 0).start()

    barrier = pltpu.get_barrier_semaphore()
    for k in range(1, n):
        pl.semaphore_signal(barrier, inc=1, device_id=(dp, peer_of(k)), device_id_type=MESH)
    pl.semaphore_wait(barrier, n - 1)

    def start_in(image):
        keep_in(image).start()
        for slot in range(1, n):
            send_in(image, slot).start()

    start_in(0)
    for layer in range(layers):
        for head in range(3 * heads):
            bqkv_ref[pl.ds(layer, 1), pl.ds(head * head_dim, head_dim)] = bias_ref[layer, head // heads, pl.ds(head % heads, 1), :]
    for which in range(1, 4):
        weight_copy(which, 0).start()
    for image in range(1, own):
        start_in(image)

    lanes = lax.broadcasted_iota(jnp.int32, (1, 256), 1)
    scale = head_dim**-0.5 * LOG2E
    pair_rows = 2 * head_dim
    last_window = width // 128 - 2
    pairs = heads // 2
    planes = width // 128

    def window(first):
        return jnp.minimum(first // 128, last_window)

    def two_planes(plane, start, size):
        return jnp.concatenate([qk_ref[plane + i, pl.ds(start, size), :] for i in range(2)], axis=1)

    def scores(pair, hh, blk, buf):
        first = (pair * 2 + hh) * head_dim
        plane = window(first)
        mask = jnp.logical_and(lanes + plane * 128 >= first, lanes + plane * 128 < first + head_dim)
        q_win = two_planes(plane, blk * qb, qb)
        q_win = jnp.where(mask, q_win, jnp.zeros_like(q_win))
        for half in range(2):
            k_win = two_planes(planes + plane, half * (seq // 2), seq // 2)
            s_ref[buf, pl.ds(half * (seq // 2), seq // 2), :] = lax.dot_general(k_win, q_win, NT, preferred_element_type=F32)

    def softmax(buf):
        half = seq // 2
        peak = jnp.maximum(s_ref[buf, pl.ds(0, half), :], s_ref[buf, pl.ds(half, half), :])
        peak = jnp.max(peak, axis=0, keepdims=True)
        total = jnp.zeros((1, qb), F32)
        probs = []
        for start, size in chunks(seq, 256):
            prob = jnp.exp2(s_ref[buf, pl.ds(start, size), :] - peak)
            probs.append(prob.astype(BF16))
            total = total + jnp.sum(prob, axis=0, keepdims=True)
        return jnp.concatenate(probs, axis=0), total

    def mix(pair, e, hh, blk, probs, total):
        v_rows = pl.ds(pl.multiple_of(pair * pair_rows + 64 * hh, 16), 80)
        values = jnp.concatenate([vt_ref[part, v_rows, :] for part in range(seq // 128)], axis=1)
        mixed = jnp.dot(values, probs, preferred_element_type=F32)
        of_ref[e, pl.ds(hh * head_dim, head_dim), pl.ds(blk * qb, qb)] = mixed[8 * hh : 8 * hh + head_dim] * (1.0 / total)

    units = [(e, hh, blk) for e in range(PAIRS) for hh in range(2) for blk in range(seq // qb)]

    def pairs_body(it, carry):
        following = jnp.minimum((it + 1) * PAIRS, pairs - 1)
        waiting = None
        for i, (e, hh, blk) in enumerate(units):
            ahead = i + AHEAD
            e1, hh1, blk1 = units[ahead % len(units)]
            scores(it * PAIRS + e1 if ahead < len(units) else following, hh1, blk1, ahead % BUFFERS)
            done = softmax(i % BUFFERS)
            if waiting:
                mix(*waiting)
            waiting = (it * PAIRS + e, e, hh, blk, *done)
        mix(*waiting)
        for e in range(PAIRS):
            at = pl.multiple_of((it * PAIRS + e) * pair_rows, 16)
            ot_ref[pl.ds(at, pair_rows), :] = of_ref[e].astype(BF16)
        return carry

    def step(g, carry):
        layer, image = g // own, lax.rem(g, own)

        @pl.when(image == 0)
        def _():
            weight_copy(0, layer).wait()

        def next_layer(which):
            @pl.when(jnp.logical_and(image == own - 1, layer < layers - 1))
            def _():
                weight_copy(which, layer + 1).start()

        def arrive(first, last):
            @pl.when(layer == 0)
            def _():
                for slot in range(first, last):
                    if slot:
                        send_in(image, slot).wait_recv()
                    else:
                        keep_in(image).wait()

        def row_of(ref, start, size):
            return ref[pl.ds(layer, 1), :][:, start : start + size]

        def qk_columns(n_at, rows_at, start, size):
            acc = lax.dot_general(from_planes(a_ref, n_at, width), wqkv_ref[pl.ds(start, size), :], NT, preferred_element_type=F32)
            acc = acc + row_of(bqkv_ref, start, size)
            if start < width:
                cols = start + lax.broadcasted_iota(jnp.int32, (1, size), 1)
                acc = acc * jnp.where(cols < width, scale, 1.0)
            to_planes(qk_ref, start, rows_at, acc.astype(BF16))

        def v_columns(t, start, size):
            first = 2 * width + start
            acc = lax.dot_general(from_planes(a_ref, pl.ds(0, rows), width), wqkv_ref[pl.ds(first, size), :], NT, preferred_element_type=F32)
            flipped = (acc + row_of(bqkv_ref, first, size)).astype(BF16).T
            for part in range(per):
                vt_ref[t * per + part, pl.ds(start, size), :] = flipped[:, part * tile : (part + 1) * tile]

        def qkv_tile(t, c):
            @pl.when(layer == 0)
            def _():
                @pl.when(t == 0)
                def _():
                    arrive(0, per)

                @pl.when(t == 1)
                def _():
                    arrive(per, n)

            half = rows // 2
            for sub in range(2):
                tokens = h_ref[image, pl.ds(t * per + sub * per // 2, per // 2)].reshape(half, width)
                normed = layer_norm(tokens, row_of(g1_ref, 0, width), row_of(s1_ref, 0, width))
                to_planes(a_ref, 0, pl.ds(sub * half, half), normed)
                qk_columns(pl.ds(sub * half, half), pl.ds(pl.multiple_of(t * rows + sub * half, half), half), 0, 512)
            for start, size in chunks(width, QKV_CHUNK):
                v_columns(t, start, size)
            for start, size in chunks(2 * width - 512, QKV_CHUNK):
                qk_columns(pl.ds(0, rows), pl.ds(pl.multiple_of(t * rows, rows), rows), 512 + start, size)
            return c

        lax.fori_loop(0, tiles, qkv_tile, 0)
        next_layer(0)
        for i, (_, hh, blk) in enumerate(units[:AHEAD]):
            scores(0, hh, blk, i)
        lax.fori_loop(0, pairs // PAIRS, pairs_body, 0)

        @pl.when(image == 0)
        def _():
            for which in range(1, 4):
                weight_copy(which, layer).wait()

        def out_tile(t):
            blocks = pl.ds(t * per, per)
            acc = jnp.dot(ot_ref[:, pl.ds(t * rows, rows)].T, wout_ref[...], preferred_element_type=F32) + row_of(bout_ref, 0, width)
            mid = (h_ref[image, blocks].reshape(rows, width).astype(F32) + acc).astype(BF16)
            h_ref[image, blocks] = mid.reshape(per, tile, width)
            to_planes(qk_ref, 0, pl.ds(t * rows, rows), layer_norm(mid, row_of(g2_ref, 0, width), row_of(s2_ref, 0, width)))

        def mlp_tile(t):
            blocks = pl.ds(t * per, per)
            for start, size in chunks(mlp, UP_CHUNK):
                acc = lax.dot_general(from_planes(qk_ref, pl.ds(t * rows, rows), width), wup_ref[pl.ds(start, size), :], NT, preferred_element_type=F32)
                to_planes(a_ref, start, pl.ds(0, rows), gelu_tanh(acc + row_of(bup_ref, start, size)).astype(BF16))
            for start, size in chunks(width, DOWN_CHUNK):
                acc = jnp.dot(from_planes(a_ref, pl.ds(0, rows), mlp), wdown_ref[:, pl.ds(start, size)], preferred_element_type=F32) + row_of(bdown_ref, start, size)
                new = h_ref[image, blocks, :, pl.ds(start, size)].reshape(rows, size).astype(F32) + acc
                h_ref[image, blocks, :, pl.ds(start, size)] = new.astype(BF16).reshape(per, tile, size)

            @pl.when(layer == layers - 1)
            def _():
                for slot in range(t * per, (t + 1) * per):
                    if slot:
                        send_out(image, slot).start()
                    else:
                        keep_out(image).start()

        for t in reversed(range(tiles)):
            out_tile(t)
        for t in reversed(range(tiles)):
            mlp_tile(t)
        for which in range(1, 4):
            next_layer(which)
        return carry

    lax.fori_loop(0, layers * own, step, 0)

    def drain(image, carry):
        keep_out(image).wait()
        for slot in range(1, n):
            send_in(image, slot).wait_send()
            send_out(image, slot).wait()
        return carry

    lax.fori_loop(0, own, drain, 0)


def solution(mesh):
    token_spec = P('dp', 'sp', None)
    n = mesh.shape['sp']

    def device_step(image_tokens, ln1_gain, ln1_shift, w_qkv, b_qkv, w_out, b_out, ln2_gain, ln2_shift, w_up, b_up, w_down, b_down):
        images, tile, width = image_tokens.shape
        layers, _, _, heads, head_dim = w_qkv.shape
        mlp = w_up.shape[2]
        own, seq = images // n, n * tile
        w_qkv = jnp.swapaxes(w_qkv.reshape(layers, width, 3 * width), 1, 2)
        w_up = jnp.swapaxes(w_up, 1, 2)
        w_out = w_out.reshape(layers, width, width)
        hbm = pl.BlockSpec(memory_space=pl.ANY)
        vmem = pl.BlockSpec(memory_space=pltpu.VMEM)
        rows = seq // 2
        return pl.pallas_call(
            functools.partial(encoder_kernel, n, layers, heads, head_dim),
            out_shape=jax.ShapeDtypeStruct(image_tokens.shape, BF16),
            in_specs=[hbm, vmem, vmem, hbm, vmem, hbm, vmem, vmem, vmem, hbm, vmem, hbm, vmem],
            out_specs=hbm,
            scratch_shapes=[
                pltpu.VMEM((own, n, tile, width), BF16),
                pltpu.VMEM((3 * width, width), BF16),
                pltpu.VMEM((width, width), BF16),
                pltpu.VMEM((mlp, width), BF16),
                pltpu.VMEM((mlp, width), BF16),
                pltpu.VMEM((2 * width // 128, seq, 128), BF16),
                pltpu.VMEM((seq // 128, width, 128), BF16),
                pltpu.VMEM((width, seq), BF16),
                pltpu.VMEM((PAIRS, 2 * head_dim, seq), F32),
                pltpu.VMEM((BUFFERS, seq, 256), F32),
                pltpu.VMEM((pl.cdiv(mlp, 128), rows, 128), BF16),
                pltpu.VMEM((layers, 3 * width), F32),
                pltpu.SemaphoreType.DMA((4,)),
                pltpu.SemaphoreType.DMA((own, n)),
                pltpu.SemaphoreType.DMA((own, n)),
                pltpu.SemaphoreType.DMA((own, n)),
                pltpu.SemaphoreType.DMA((own, n)),
            ],
            compiler_params=pltpu.CompilerParams(vmem_limit_bytes=VMEM_LIMIT, collective_id=0, has_side_effects=True),
            name='encoder',
        )(
            image_tokens, ln1_gain, ln1_shift, w_qkv, b_qkv, w_out, b_out,
            ln2_gain, ln2_shift, w_up, b_up, w_down, b_down,
        )

    return jax.shard_map(device_step, mesh=mesh, in_specs=(token_spec,) + (P(),) * 12, out_specs=token_spec, check_vma=False)
```
